512 devices in a mesh: atoms: 32 (over z, x), modes: 16 (over y, core).
Axes of the slice: x: 4, y: 8, z: 8, core: 2. Of those that a mesh axis runs over, the one named last changes fastest.
Arguments:
- subspace: float32 [768, 65536], P('modes', 'atoms'), may hold values from -100 to 100
- applied: float32 [768, 65536], P('modes', 'atoms'), may hold values from -300 to 300
Outputs:
- ortho_basis: float32 [768, 65536], P('modes', 'atoms')
- projected: float32 [768, 768], P('modes')
The draws below stay inside these ranges and needn't reach their ends.
All inputs are finite; a program needn't handle non-finite values.
Results may differ from the reference program's by a relative error of at most 0.00025.
Values sent between devices are 32-bit elements; how exact they have to be, the bound alone decides.
A program may use at most 64 MiB of HBM per device.

```python
import math
import jax
import jax.numpy as jnp
from jax import lax

K = 768
NROWS = 65536


def mixed_subspace(key):
    keys = jax.random.split(jax.random.fold_in(key, 11), 3)
    normals = jax.random.truncated_normal(keys[0], -6.0, 6.0, (NROWS, K), jnp.float32)
    weights = jax.random.truncated_normal(keys[1], -4.0, 4.0, (K, K), jnp.float32)
    mixing = jnp.eye(K, dtype=jnp.float32) + 0.5 * weights / math.sqrt(K)
    col_scale = jnp.exp(jax.random.uniform(keys[2], (K,), jnp.float32, 0.0, math.log(10.0)))
    mixed = jnp.dot(normals, mixing, precision=lax.Precision.HIGHEST)
    return jnp.clip(mixed * col_scale[None, :], -100.0, 100.0)


def draw_subspace(key, part):
    return mixed_subspace(key).T


def draw_applied(key, part):
    vectors = mixed_subspace(key)
    keys = jax.random.split(jax.random.fold_in(key, 23), 3)
    eigen_part = jax.random.uniform(keys[0], (K,), jnp.float32, -1.0, 2.0)
    weights = jax.random.truncated_normal(keys[1], -4.0, 4.0, (K, K), jnp.float32)
    coupling = jnp.diag(eigen_part) + 0.3 * (weights + weights.T) / math.sqrt(2.0 * K)
    jitter = jax.random.truncated_normal(keys[2], -6.0, 6.0, (NROWS, K), jnp.float32)
    result = jnp.dot(vectors, coupling, precision=lax.Precision.HIGHEST) + 2.0 * jitter
    return jnp.clip(result, -300.0, 300.0).T


def setup_inputs(seed: int = 0) -> dict:
    key_list = jax.random.split(jax.random.key(seed), 3)
    return {
        "subspace": draw_subspace(jax.random.fold_in(key_list[2], 71), 0),
        "applied": draw_applied(jax.random.fold_in(key_list[2], 71), 0),
    }


def reference(subspace, applied):
    highest = lax.Precision.HIGHEST
    gram = jnp.dot(subspace.astype(jnp.float32), subspace.T.astype(jnp.float32), precision=highest, preferred_element_type=jnp.float32) / NROWS
    cross = jnp.dot(subspace.astype(jnp.float32), applied.T.astype(jnp.float32), precision=highest, preferred_element_type=jnp.float32) / NROWS
    factor = jnp.linalg.cholesky(gram)
    identity = jnp.eye(K, dtype=gram.dtype)
    inv_lower = lax.linalg.triangular_solve(factor, identity, left_side=True, lower=True)
    inv_upper = inv_lower.T
    ortho_basis = jnp.dot(inv_lower.astype(jnp.float32), subspace.astype(jnp.float32), precision=highest, preferred_element_type=jnp.float32)
    half_proj = jnp.dot(inv_lower.astype(jnp.float32), cross.astype(jnp.float32), precision=highest, preferred_element_type=jnp.float32)
    projected = jnp.dot(half_proj.astype(jnp.float32), inv_upper.astype(jnp.float32), precision=highest, preferred_element_type=jnp.float32)
    return (ortho_basis, projected)
```

```python
import jax
import jax.numpy as jnp
from jax import lax
from jax.experimental import pallas as pl
from jax.experimental.pallas import tpu as pltpu
from jax.sharding import PartitionSpec as P


def in_blocks(value, dim, count):
    lengths = value.shape
    tiles = value.reshape(*lengths[:dim], count, lengths[dim] // count, *lengths[dim + 1 :])
    return jnp.moveaxis(tiles, dim, 0)


def sum_at_owner(value, axis, dim):
    count = lax.axis_size(axis)
    tiles = lax.all_to_all(in_blocks(value, dim, count), axis, 0, 0, tiled=True)
    return jnp.sum(tiles, axis=0)


def rows_for(lines, count):
    spare = -len(lines) % count
    return jnp.pad(lines, [(0, spare)] + [(0, 0)] * (lines.ndim - 1))


def copy_for_each(value, axis):
    count = lax.axis_size(axis)
    return lax.all_to_all(
        jnp.broadcast_to(value[None], (count, *value.shape)), axis, 0, 0, tiled=True
    )


def laid_out(tiles, dim):
    lengths = list(tiles.shape[1:])
    lengths[dim] *= tiles.shape[0]
    return jnp.moveaxis(tiles, 0, dim).reshape(lengths)


def collect(value, axis, dim):
    tiles = copy_for_each(value, axis)
    return laid_out(tiles, dim)


def nested_sum(value, axes):
    own = sum_at_owner(rows_for(value, lax.axis_size(axes)), axes, 0)
    whole = collect(own, axes, 0)
    return whole[: len(value)].reshape(value.shape)


def together(arrays, axis):
    ends = [0]
    for a in arrays:
        ends.append(ends[-1] + a.size)
    running = nested_sum(jnp.concatenate([a.ravel() for a in arrays]), axis)
    return tuple((running[b:e].reshape(a.shape) for a, b, e in zip(arrays, ends, ends[1:])))


def sent_together(arrays, axis, dim, along):
    both = jnp.concatenate(arrays, axis=along)
    out, at, gathered = (lax.all_gather(both, axis, axis=dim, tiled=True), 0, [])
    for a in arrays:
        gathered.append(lax.slice_in_dim(out, at, at + a.shape[along], axis=along))
        at += a.shape[along]
    return tuple(gathered)


def contract_cols(left, right):
    return lax.dot_general(
        left,
        right,
        (((1,), (1,)), ((), ())),
        precision=lax.Precision.HIGHEST,
        preferred_element_type=jnp.float32,
    )


def matmul(left, right):
    return jnp.dot(left, right, precision=lax.Precision.HIGHEST, preferred_element_type=jnp.float32)


B = 128
HI = lax.Precision.HIGHEST


def lane_bcast(v, j):
    return jnp.broadcast_to(v[:, j : j + 1], v.shape)


def row_bcast(v, j):
    return jnp.broadcast_to(v[j : j + 1, :], v.shape)


def factor_block(d_ref, m_ref):
    lane = lax.broadcasted_iota(jnp.int32, (8, B), 1)
    sub = lax.broadcasted_iota(jnp.int32, (8, B), 0)
    for s in range(B // 8):
        m_ref[8 * s : 8 * s + 8, :] = jnp.where(lane == sub + 8 * s, 1.0, 0.0)
    groups = B // 8
    for s in range(groups):
        r0 = 8 * s
        d = d_ref[r0 : r0 + 8, :]
        m = m_ref[r0 : r0 + 8, :]
        col = [lane_bcast(d, r0 + k) for k in range(8)]
        last = s == groups - 1
        if not last:
            nd = d_ref[r0 + 8 : r0 + 16, :]
            nm = m_ref[r0 + 8 : r0 + 16, :]
            ncol = [lane_bcast(nd, r0 + k) for k in range(8)]
        scale = None
        for j in range(8):
            pivot = row_bcast(col[j], j)
            inv = 1.0 / pivot
            root = lax.rsqrt(pivot)
            scale = root if scale is None else jnp.where(sub >= j, root, scale)
            dj = row_bcast(d, j) * inv
            mj = row_bcast(m, j) * inv
            for k in range(j + 1, 8):
                f = row_bcast(col[k], j) * inv
                if j < 7:
                    col[k] = col[k] - col[j] * f
                if not last:
                    ncol[k] = ncol[k] - ncol[j] * f
            below = jnp.where(sub > j, col[j], 0.0)
            if j < 7:
                d = d - below * dj
                m = m - below * mj
            if not last:
                nd = nd - ncol[j] * dj
                nm = nm - ncol[j] * mj
        d = d * scale
        m = m * scale
        m_ref[r0 : r0 + 8, :] = m
        if not last:
            d_ref[r0 + 8 : r0 + 16, :] = nd
            m_ref[r0 + 8 : r0 + 16, :] = nm
        if s < groups - 2:
            t = d.T
            drow = [row_bcast(d, j) for j in range(8)]
            mrow = [row_bcast(m, j) for j in range(8)]
            for g in range(s + 2, groups):
                tg = t[8 * g : 8 * g + 8, :]
                xd = d_ref[8 * g : 8 * g + 8, :]
                xm = m_ref[8 * g : 8 * g + 8, :]
                for j in range(8):
                    c = jnp.broadcast_to(tg[:, j : j + 1], (8, B))
                    xd = xd - c * drow[j]
                    xm = xm - c * mrow[j]
                d_ref[8 * g : 8 * g + 8, :] = xd
                m_ref[8 * g : 8 * g + 8, :] = xm


def dot(a, b, dims):
    return lax.dot_general(a, b, (dims, ((), ())), precision=HI, preferred_element_type=jnp.float32)


def invert_lower(z_ref, d_ref, m_ref):
    n = z_ref.shape[0]
    steps = n // B

    @pl.loop(0, steps)
    def _(k):
        k0 = pl.multiple_of(k * B, B)
        d_ref[...] = z_ref[pl.ds(k0, B), pl.ds(k0, B)]
        factor_block(d_ref, m_ref)
        for kk in range(steps):
            @pl.when(k == kk)
            def _():
                lo, hi = kk * B, (kk + 1) * B
                m = m_ref[...]
                if kk:
                    z_ref[lo:hi, :lo] = dot(m, z_ref[lo:hi, :lo], ((1,), (0,)))
                z_ref[lo:hi, lo:hi] = m
                if hi < n:
                    r = dot(m, z_ref[lo:hi, hi:], ((1,), (0,)))
                    z_ref[hi:, lo:hi] = jnp.zeros((n - hi, B), jnp.float32)
                    z_ref[lo:hi, hi:] = jnp.zeros((B, n - hi), jnp.float32)
                    rt = r.T
                    z_ref[hi:, :hi] -= dot(rt, z_ref[lo:hi, :hi], ((1,), (0,)))
                    z_ref[hi:, hi:] -= dot(rt, r, ((1,), (0,)))


def chol_kernel(g_ref, z_ref, d_ref, m_ref):
    z_ref[...] = g_ref[...]
    invert_lower(z_ref, d_ref, m_ref)


def inverse_factor(gram):
    n = gram.shape[0]
    vm = pl.BlockSpec(memory_space=pltpu.VMEM)
    return pl.pallas_call(
        chol_kernel,
        out_shape=jax.ShapeDtypeStruct((n, n), jnp.float32),
        in_specs=[vm], out_specs=vm,
        scratch_shapes=[pltpu.VMEM((B, B), jnp.float32), pltpu.VMEM((B, B), jnp.float32)],
        compiler_params=pltpu.CompilerParams(vmem_limit_bytes=48 * 2**20),
        name="inverse_factor",
    )(gram)


def per_device(subspace, applied):
    mode_width = subspace.shape[0]
    row_total = subspace.shape[1] * lax.axis_size("atoms")
    mode_start = lax.axis_index("modes") * mode_width
    full_modes = lax.all_gather(subspace, "modes", axis=0, tiled=True)
    gram_part = contract_cols(subspace, full_modes) / row_total
    crosst_part = contract_cols(applied, full_modes) / row_total
    gram_rows, crosst_rows = together((gram_part, crosst_part), "atoms")
    gram_full, crosst_full = sent_together((gram_rows, crosst_rows), "modes", 0, 1)
    inv_lower = inverse_factor(gram_full)
    inv_upper = inv_lower.T
    lower_rows = lax.dynamic_slice_in_dim(inv_lower, mode_start, mode_width, 0)
    ortho_basis = matmul(lower_rows, full_modes)
    projected = matmul(matmul(lower_rows, crosst_full.T), inv_upper)
    return (ortho_basis, projected)


def solution(mesh):
    return jax.shard_map(
        per_device,
        mesh=mesh,
        in_specs=(P("modes", "atoms"), P("modes", "atoms")),
        out_specs=(P("modes", "atoms"), P("modes", None)),
        check_vma=False,
    )
```

```python
import functools

import jax
import jax.numpy as jnp
from jax import lax
from jax.experimental import pallas as pl
from jax.experimental.pallas import tpu as pltpu
from jax.sharding import PartitionSpec as P

MESH = pl.DeviceIdType.MESH
NX, NY, NZ = 4, 8, 8
UNITS = 12
UNIT_PLACES = [(i, p) for i in range(6) for p in range(i // 2 + 1)]
B = 128
HI = lax.Precision.HIGHEST


def lane_bcast(v, j):
    return jnp.broadcast_to(v[:, j : j + 1], v.shape)


def row_bcast(v, j):
    return jnp.broadcast_to(v[j : j + 1, :], v.shape)


def factor_block(d_ref, m_ref):
    lane = lax.broadcasted_iota(jnp.int32, (8, B), 1)
    sub = lax.broadcasted_iota(jnp.int32, (8, B), 0)
    for s in range(B // 8):
        m_ref[8 * s : 8 * s + 8, :] = jnp.where(lane == sub + 8 * s, 1.0, 0.0)
    groups = B // 8
    for s in range(groups):
        r0 = 8 * s
        d = d_ref[r0 : r0 + 8, :]
        m = m_ref[r0 : r0 + 8, :]
        col = [lane_bcast(d, r0 + k) for k in range(8)]
        last = s == groups - 1
        if not last:
            nd = d_ref[r0 + 8 : r0 + 16, :]
            nm = m_ref[r0 + 8 : r0 + 16, :]
            ncol = [lane_bcast(nd, r0 + k) for k in range(8)]
        scale = None
        for j in range(8):
            pivot = row_bcast(col[j], j)
            inv = 1.0 / pivot
            root = lax.rsqrt(pivot)
            scale = root if scale is None else jnp.where(sub >= j, root, scale)
            dj = row_bcast(d, j) * inv
            mj = row_bcast(m, j) * inv
            for k in range(j + 1, 8):
                f = row_bcast(col[k], j) * inv
                if j < 7:
                    col[k] = col[k] - col[j] * f
                if not last:
                    ncol[k] = ncol[k] - ncol[j] * f
            below = jnp.where(sub > j, col[j], 0.0)
            if j < 7:
                d = d - below * dj
                m = m - below * mj
            if not last:
                nd = nd - ncol[j] * dj
                nm = nm - ncol[j] * mj
        d = d * scale
        m = m * scale
        m_ref[r0 : r0 + 8, :] = m
        if not last:
            d_ref[r0 + 8 : r0 + 16, :] = nd
            m_ref[r0 + 8 : r0 + 16, :] = nm
        if s < groups - 2:
            t = d.T
            drow = [row_bcast(d, j) for j in range(8)]
            mrow = [row_bcast(m, j) for j in range(8)]
            for g in range(s + 2, groups):
                tg = t[8 * g : 8 * g + 8, :]
                xd = d_ref[8 * g : 8 * g + 8, :]
                xm = m_ref[8 * g : 8 * g + 8, :]
                for j in range(8):
                    c = jnp.broadcast_to(tg[:, j : j + 1], (8, B))
                    xd = xd - c * drow[j]
                    xm = xm - c * mrow[j]
                d_ref[8 * g : 8 * g + 8, :] = xd
                m_ref[8 * g : 8 * g + 8, :] = xm


def dot(a, b, dims):
    return lax.dot_general(a, b, (dims, ((), ())), precision=HI, preferred_element_type=jnp.float32)


def invert_lower(z_ref, d_ref, m_ref):
    n = z_ref.shape[0]
    steps = n // B

    @pl.loop(0, steps)
    def _(k):
        k0 = pl.multiple_of(k * B, B)
        d_ref[...] = z_ref[pl.ds(k0, B), pl.ds(k0, B)]
        factor_block(d_ref, m_ref)
        for kk in range(steps):
            @pl.when(k == kk)
            def _():
                lo, hi = kk * B, (kk + 1) * B
                m = m_ref[...]
                if kk:
                    z_ref[lo:hi, :lo] = dot(m, z_ref[lo:hi, :lo], ((1,), (0,)))
                z_ref[lo:hi, lo:hi] = m
                if hi < n:
                    r = dot(m, z_ref[hi:, lo:hi], ((1,), (1,)))
                    z_ref[hi:, lo:hi] = jnp.zeros((n - hi, B), jnp.float32)
                    z_ref[lo:hi, hi:] = jnp.zeros((B, n - hi), jnp.float32)
                    rt = r.T
                    z_ref[hi:, :hi] -= dot(rt, z_ref[lo:hi, :hi], ((1,), (0,)))
                    z_ref[hi:, hi:] -= dot(rt, r, ((1,), (0,)))


def copy_to(src, dst, send, recv, device):
    return pltpu.make_async_remote_copy(
        src_ref=src, dst_ref=dst, send_sem=send, recv_sem=recv, device_id=device, device_id_type=MESH
    )


def kernel(
    s_hbm, a_hbm, ortho_ref, proj_ref,
    s_all, a_own, g_part, g_x, g_z, g_all, c_part, c_x, c_z, c_all, z_ref, ct_ref, d_ref, m_ref,
    load_sem, ring_send, ring_recv, twin_send, twin_recv,
    gx_send, gx_recv, gz_send, gz_recv, gy_send, gy_recv, gg_send, gg_recv, gt_send, gt_recv,
    cx_send, cx_recv, cz_send, cz_recv, cy_send, cy_recv, cg_send, cg_recv, ct_send, ct_recv,
):
    atom, mode = lax.axis_index("atoms"), lax.axis_index("modes")
    z, x = atom // NX, atom % NX
    y, core = mode // 2, mode % 2
    rows = s_hbm.shape[0]
    half_rows = rows // 2
    total = s_hbm.shape[1] * NX * NZ
    wide = s_hbm.shape[1]

    def at_x(d):
        return (z * NX + (x + d) % NX, mode)

    def at_y(d):
        return (atom, ((y + d) % NY) * 2 + core)

    def at_z(d):
        return (((z + d) % NZ) * NX + x, mode)

    twin = (atom, y * 2 + (1 - core))

    own_s = pltpu.make_async_copy(
        s_hbm, s_all.at[pl.ds(pl.multiple_of(mode * rows, 8), rows), :], load_sem.at[0]
    )
    own_a = pltpu.make_async_copy(a_hbm, a_own, load_sem.at[1])
    own_s.start()
    own_a.start()
    barrier = pltpu.get_barrier_semaphore()
    peers = [at_x(d) for d in range(1, NX)] + [at_y(d) for d in range(1, NY)]
    peers += [at_z(d) for d in range(1, NZ)] + [twin]
    for peer in peers:
        pl.semaphore_signal(barrier, inc=1, device_id=peer, device_id_type=MESH)
    own_s.wait()
    pl.semaphore_wait(barrier, len(peers))

    pending = []

    def piece(back, which, q):
        start = (((y + NY - back) % NY) * 2 + which) * rows + q * half_rows
        return s_all.at[pl.ds(pl.multiple_of(start, 8), half_rows), :]

    def ring(way, hop, q):
        back = hop if way == 0 else (NY - hop) % NY
        ref = piece(back, core, q)
        return copy_to(
            ref, ref, ring_send.at[way, hop, q], ring_recv.at[way, hop, q], at_y(1 if way == 0 else NY - 1)
        )

    def ring_in(way, hop, q):
        back = hop + 1 if way == 0 else NY - hop - 1
        ref = piece(back, core, q)
        return copy_to(
            ref, ref, ring_send.at[way, hop, q], ring_recv.at[way, hop, q], at_y(1 if way == 0 else NY - 1)
        )

    def to_twin(back, q):
        ref = piece(back, core, q)
        return copy_to(ref, ref, twin_send.at[back, q], twin_recv.at[back, q], twin)

    def from_twin(back, q):
        ref = piece(back, 1 - core, q)
        return copy_to(ref, ref, twin_send.at[back, q], twin_recv.at[back, q], twin)

    def go(copy):
        copy.start()
        pending.append(copy)

    for q in range(2):
        for way in range(2):
            go(ring(way, 0, q))
    for q in range(2):
        go(to_twin(0, q))
    for hop in range(1, 4):
        for q in range(2):
            for way in range(2):
                ring_in(way, hop - 1, q).wait_recv()
                if hop < 3 or q == way:
                    go(ring(way, hop, q))
                go(to_twin(hop if way == 0 else NY - hop, q))
    for way in range(2):
        ring_in(way, 3, way).wait_recv()
        go(to_twin(4, way))
    own_a.wait()
    for back in (0, 1, 7, 2, 6, 3, 5, 4):
        for q in range(2):
            from_twin(back, q).wait_recv()

    def least(n):
        return (mode >= n).astype(jnp.int32)

    block = least(1) + least(2) + least(4) + least(6) + least(9)
    first = least(1) + least(2) + 2 * least(4) + 2 * least(6) + 3 * least(9)
    pair = jnp.minimum(mode - first, 2)
    row0 = pl.multiple_of(block * 128, 128)
    col0 = pl.multiple_of(pair * 256, 128)
    step = 256

    def gram_step(i, acc):
        k = pl.ds(pl.multiple_of(i * step, 128), step)
        return acc + dot(s_all[pl.ds(row0, 128), k], s_all[pl.ds(col0, 256), k], ((1,), (1,)))

    unit = lax.fori_loop(0, wide // step, gram_step, jnp.zeros((128, 256), jnp.float32))
    for t in range(32):
        r, h = 8 * (t // 2), 128 * (t % 2)
        g_part[t // 8, t % 8] = unit[r : r + 8, h : h + 128]

    def x_sum(part, landing, send, recv):
        out = [copy_to(part.at[(x + d) % NX], landing.at[d - 1], send.at[d - 1], recv.at[d - 1], at_x(d)) for d in range(1, NX)]

        def finish(spread):
            for c in out:
                c.wait_recv()
            spread[z] = (part[x] + landing[0] + landing[1] + landing[2]) * (1.0 / total)

        for c in out:
            go(c)
        return finish

    def z_sum(spread, send, recv):
        for d in range(1, NZ):
            go(copy_to(spread.at[z], spread.at[z], send.at[d - 1], recv.at[d - 1], at_z(d)))

        def finish(place):
            for d in range(1, NZ):
                ref = spread.at[(z + NZ - d) % NZ]
                copy_to(ref, ref, send.at[d - 1], recv.at[d - 1], at_z(d)).wait_recv()
            value = spread[0]
            for i in range(1, NZ):
                value = value + spread[i]
            place[core, y, x] = value

        return finish

    def y_spread(place, send, recv, count):
        def out(d):
            ref = place.at[core, y, x]
            return copy_to(ref, ref, send.at[d - 1], recv.at[d - 1], at_y(d))

        def start():
            for d in range(1, NY):
                out(d).start()

        def finish():
            for d in range(1, NY):
                def wait():
                    ref = place.at[core, (y + NY - d) % NY, x]
                    copy_to(ref, ref, send.at[d - 1], recv.at[d - 1], at_y(d)).wait_recv()
                if count < NY:
                    pl.when((y + NY - d) % NY < count)(wait)
                else:
                    wait()

        def sent():
            for d in range(1, NY):
                out(d).wait_send()

        if count < NY:
            pl.when(y < count)(start)
        else:
            start()
        return finish, sent

    def x_spread(place, send, recv, count):
        def ref(at):
            return place.at[core, pl.ds(0, count), at]

        for d in range(1, NX):
            go(copy_to(ref(x), ref(x), send.at[d - 1], recv.at[d - 1], at_x(d)))

        def finish():
            for d in range(1, NX):
                r = ref((x + NX - d) % NX)
                copy_to(r, r, send.at[d - 1], recv.at[d - 1], at_x(d)).wait_recv()

        return finish

    def twin_spread(place, send, recv, count):
        def ref(which):
            return place.at[which, pl.ds(0, count)]

        go(copy_to(ref(core), ref(core), send.at[0], recv.at[0], twin))

        def finish():
            copy_to(ref(1 - core), ref(1 - core), send.at[0], recv.at[0], twin).wait_recv()

        return finish

    g_x_done = x_sum(g_part, g_x, gx_send, gx_recv)

    def cross_step(i, acc):
        k = pl.ds(pl.multiple_of(i * step, 128), step)
        return acc + dot(a_own[:, k], s_all[:, k], ((1,), (1,)))

    crosst = lax.fori_loop(0, wide // step, cross_step, jnp.zeros((rows, s_all.shape[0]), jnp.float32))
    for t in range(36):
        r, h = 8 * (t // 6), 128 * (t % 6)
        c_part[t // 9, t % 9] = crosst[r : r + 8, h : h + 128]

    g_x_done(g_z)
    g_z_done = z_sum(g_z, gz_send, gz_recv)
    c_x_done = x_sum(c_part, c_x, cx_send, cx_recv)
    g_z_done(g_all)
    g_y_done, g_y_sent = y_spread(g_all, gy_send, gy_recv, UNITS // 2)
    c_x_done(c_z)
    c_z_done = z_sum(c_z, cz_send, cz_recv)
    g_y_done()
    g_s_done = x_spread(g_all, gg_send, gg_recv, UNITS // 2)
    c_z_done(c_all)
    c_y_done, c_y_sent = y_spread(c_all, cy_send, cy_recv, NY)
    g_s_done()
    g_t_done = twin_spread(g_all, gt_send, gt_recv, UNITS // 2)
    g_t_done()
    for u, (i, p) in enumerate(UNIT_PLACES):
        for t in range(32):
            r, h = i * 128 + 8 * (t // 2), p * 256 + 128 * (t % 2)
            z_ref[r : r + 8, h : h + 128] = g_all[u % 2, u // 2, t // 8, t % 8]
    c_y_done()
    c_s_done = x_spread(c_all, cg_send, cg_recv, NY)

    invert_lower(z_ref, d_ref, m_ref)

    c_s_done()
    c_t_done = twin_spread(c_all, ct_send, ct_recv, NY)
    lower = z_ref[pl.ds(pl.multiple_of(mode * rows, 8), rows), :]

    @pl.loop(0, wide // step)
    def _(i):
        k = pl.ds(pl.multiple_of(i * step, 128), step)
        ortho_ref[:, k] = dot(lower, s_all[:, k], ((1,), (0,)))

    c_t_done()
    for m in range(2 * NY):
        for t in range(36):
            r, h = m * rows + 8 * (t // 6), 128 * (t % 6)
            ct_ref[r : r + 8, h : h + 128] = c_all[m % 2, m // 2, t // 9, t % 9]
    half = dot(lower, ct_ref[...], ((1,), (1,)))
    proj_ref[...] = dot(half, z_ref[...], ((1,), (1,)))
    for c in pending:
        c.wait_send()
    pl.when(y < UNITS // 2)(g_y_sent)
    c_y_sent()


def per_device(subspace, applied):
    rows, wide = subspace.shape
    n = rows * lax.axis_size("modes")
    f32 = jnp.float32
    dma = pltpu.SemaphoreType.DMA
    exchange = lambda: [dma((NX - 1,))] * 2 + [dma((NZ - 1,))] * 2 + [dma((NY - 1,))] * 2 + [dma((NX - 1,))] * 2 + [dma((1,))] * 2
    return pl.pallas_call(
        kernel,
        out_shape=(
            jax.ShapeDtypeStruct((rows, wide), f32),
            jax.ShapeDtypeStruct((rows, n), f32),
        ),
        in_specs=[pl.BlockSpec(memory_space=pl.ANY)] * 2,
        out_specs=[pl.BlockSpec(memory_space=pltpu.VMEM)] * 2,
        scratch_shapes=[
            pltpu.VMEM((n, wide), f32),
            pltpu.VMEM((rows, wide), f32),
            pltpu.VMEM((NX, 8, 8, 128), f32),
            pltpu.VMEM((NX - 1, 8, 8, 128), f32),
            pltpu.VMEM((NZ, 8, 8, 128), f32),
            pltpu.VMEM((2, UNITS // 2 + 2, NX, 8, 8, 128), f32),
            pltpu.VMEM((NX, 9, 8, 128), f32),
            pltpu.VMEM((NX - 1, 9, 8, 128), f32),
            pltpu.VMEM((NZ, 9, 8, 128), f32),
            pltpu.VMEM((2, NY, NX, 9, 8, 128), f32),
            pltpu.VMEM((n, n), f32),
            pltpu.VMEM((n, n), f32),
            pltpu.VMEM((B, B), f32),
            pltpu.VMEM((B, B), f32),
            dma((2,)),
            dma((2, 4, 2)), dma((2, 4, 2)), dma((NY, 2)), dma((NY, 2)),
            *exchange(), *exchange(),
        ],
        compiler_params=pltpu.CompilerParams(
            collective_id=0, has_side_effects=True, vmem_limit_bytes=56 * 2**20
        ),
        name="cholesky_qr",
    )(subspace, applied)


def solution(mesh):
    return jax.shard_map(
        per_device,
        mesh=mesh,
        in_specs=(P("modes", "atoms"), P("modes", "atoms")),
        out_specs=(P("modes", "atoms"), P("modes", None)),
        check_vma=False,
    )
```

```python
import jax
import jax.numpy as jnp
from jax import lax
from jax.experimental import pallas as pl
from jax.experimental.pallas import tpu as pltpu
from jax.sharding import PartitionSpec as P

MESH = pl.DeviceIdType.MESH
NX, NY, NZ = 4, 8, 8
GT, CT = 7, 9

B = 128
PANEL, STRIP = 32, 16
HI = lax.Precision.HIGHEST


def lane_bcast(v, j):
    return jnp.broadcast_to(v[:, j : j + 1], v.shape)


def row_bcast(v, j):
    return jnp.broadcast_to(v[j : j + 1, :], v.shape)


def factor_block(d_ref, m_ref):
    lane = lax.broadcasted_iota(jnp.int32, (8, B), 1)
    sub = lax.broadcasted_iota(jnp.int32, (8, B), 0)
    for s in range(B // 8):
        m_ref[8 * s : 8 * s + 8, :] = jnp.where(lane == sub + 8 * s, 1.0, 0.0)
    n = PANEL // 8
    for p0 in range(0, B, PANEL):
        d = [d_ref[p0 + 8 * g : p0 + 8 * g + 8, :] for g in range(n)]
        m = [m_ref[p0 + 8 * g : p0 + 8 * g + 8, :] for g in range(n)]
        for s0 in range(0, n, STRIP // 8):
            r0 = p0 + 8 * s0
            col = {g: [lane_bcast(d[g], r0 + k) for k in range(STRIP)] for g in range(s0, n)}
            scale = {}
            for j in range(STRIP):
                s, jj = s0 + j // 8, j % 8
                pivot = row_bcast(col[s][j], jj)
                inv = 1.0 / pivot
                root = lax.rsqrt(pivot)
                scale[s] = root if jj == 0 else jnp.where(sub >= jj, root, scale[s])
                dj = row_bcast(d[s], jj) * inv
                mj = row_bcast(m[s], jj) * inv
                for k in range(j + 1, STRIP):
                    f = row_bcast(col[s][k], jj) * inv
                    for g in range(s, n):
                        if g > s or jj < 7:
                            col[g][k] = col[g][k] - col[g][j] * f
                for g in range(s, n):
                    c = col[g][j]
                    if g == s:
                        if jj == 7:
                            continue
                        c = jnp.where(sub > jj, c, 0.0)
                    d[g] = d[g] - c * dj
                    m[g] = m[g] - c * mj
            for s in range(s0, s0 + STRIP // 8):
                d[s] = d[s] * scale[s]
                m[s] = m[s] * scale[s]
        for g in range(n):
            m_ref[p0 + 8 * g : p0 + 8 * g + 8, :] = m[g]
        if p0 + PANEL < B:
            r = jnp.concatenate(d, axis=0)
            q = jnp.concatenate(m, axis=0)
            t = r.T[p0 + PANEL :, :]
            d_ref[p0 + PANEL :, :] -= dot(t, r, ((1,), (0,)))
            m_ref[p0 + PANEL :, :] -= dot(t, q, ((1,), (0,)))


def dot(a, b, dims):
    return lax.dot_general(a, b, (dims, ((), ())), precision=HI, preferred_element_type=jnp.float32)


def dot3(a, b, dims):
    bf, f32 = jnp.bfloat16, jnp.float32
    ah, bh = a.astype(bf), b.astype(bf)
    al, bl = (a - ah.astype(f32)).astype(bf), (b - bh.astype(f32)).astype(bf)

    def one(p, q):
        return lax.dot_general(p, q, (dims, ((), ())), preferred_element_type=f32)

    return one(ah, bh) + (one(al, bh) + one(ah, bl))


def invert_lower(z_ref, d_ref, m_ref, between):
    n = z_ref.shape[0]
    steps = n // B
    row = lax.broadcasted_iota(jnp.int32, (B, B), 0)
    lane = lax.broadcasted_iota(jnp.int32, (B, B), 1)

    @pl.loop(0, steps)
    def _(k):
        between(k)
        k0 = pl.multiple_of(k * B, B)
        d = z_ref[pl.ds(k0, B), pl.ds(k0, B)]
        d_ref[...] = jnp.where(row >= lane, d, d.T)
        factor_block(d_ref, m_ref)
        for kk in range(steps):

            @pl.when(k == kk)
            def _():
                lo, hi = kk * B, (kk + 1) * B
                m = m_ref[...]
                if hi < n:
                    r = dot(m, z_ref[hi:, lo:hi], ((1,), (1,)))
                    rt = r.T
                    for c in range(hi, n, 2 * B):
                        e = min(c + 2 * B, n)
                        z_ref[c:, c:e] -= dot(rt[c - hi :], r[:, c - hi : e - hi], ((1,), (0,)))
                    z_ref[hi:, lo:hi] = jnp.zeros((n - hi, B), jnp.float32)
                    z_ref[lo:hi, hi:] = jnp.zeros((B, n - hi), jnp.float32)
                if kk:
                    z_ref[lo:hi, :lo] = dot(m, z_ref[lo:hi, :lo], ((1,), (0,)))
                z_ref[lo:hi, lo:hi] = m
                if hi < n:
                    z_ref[hi:, :hi] -= dot(rt, z_ref[lo:hi, :hi], ((1,), (0,)))


def copy_to(src, dst, send, recv, device):
    return pltpu.make_async_remote_copy(
        src_ref=src, dst_ref=dst, send_sem=send, recv_sem=recv, device_id=device, device_id_type=MESH
    )


class Exchange:
    def __init__(self, out, arriving):
        self.out, self.arriving = out, arriving

    def start(self):
        for c in self.out():
            c.start()

    def arrive(self):
        for c in self.arriving():
            c.wait_recv()

    def sent(self):
        for c in self.out():
            c.wait_send()


def kernel(
    s_hbm, a_hbm, ortho_ref, proj_ref,
    s_all, a_own, g_part, g_x, g_z, g_all, c_part, c_x, c_z, c_all, z_ref, ct_ref, d_ref, m_ref,
    load_sem, ring_send, ring_recv, twin_send, twin_recv, *sems,
):
    atom, mode = lax.axis_index("atoms"), lax.axis_index("modes")
    z, x = atom // NX, atom % NX
    y, core = mode // 2, mode % 2
    rows, wide = s_hbm.shape
    half_rows = rows // 2
    chip_rows = 2 * rows
    total = wide * NX * NZ

    def at_x(d):
        return (z * NX + (x + d) % NX, mode)

    def at_y(d):
        return (atom, ((y + d) % NY) * 2 + core)

    def at_z(d):
        return (((z + d) % NZ) * NX + x, mode)

    twin = (atom, y * 2 + (1 - core))

    barrier = pltpu.get_barrier_semaphore()
    peers = [at_z(d) for d in range(1, NZ)] + [at_y(d) for d in range(1, NY)]
    peers += [at_x(d) for d in range(1, NX)] + [twin]
    for peer in peers:
        pl.semaphore_signal(barrier, inc=1, device_id=peer, device_id_type=MESH)
    own_s = pltpu.make_async_copy(
        s_hbm, s_all.at[pl.ds(pl.multiple_of(mode * rows, 8), rows), :], load_sem.at[0]
    )
    own_a = pltpu.make_async_copy(a_hbm, a_own, load_sem.at[1])
    own_s.start()
    own_a.start()
    own_s.wait()
    pl.semaphore_wait(barrier, len(peers))

    pending = []

    def go(copy):
        copy.start()
        pending.append(copy)

    def piece(back, which, q):
        start = (((y + NY - back) % NY) * 2 + which) * rows + q * half_rows
        return s_all.at[pl.ds(pl.multiple_of(start, 8), half_rows), :]

    def ring(way, hop, q, back):
        ref = piece(back, core, q)
        sems = ring_send.at[way, hop, q], ring_recv.at[way, hop, q]
        return copy_to(ref, ref, *sems, at_y(1 if way == 0 else NY - 1))

    def ring_out(way, hop, q):
        return ring(way, hop, q, hop if way == 0 else (NY - hop) % NY)

    def ring_in(way, hop, q):
        return ring(way, hop, q, hop + 1 if way == 0 else NY - hop - 1)

    def to_twin(back, q, which):
        ref = piece(back, which, q)
        return copy_to(ref, ref, twin_send.at[back, q], twin_recv.at[back, q], twin)

    def pass_on(hop):
        for q in range(2):
            for way in range(2):
                ring_in(way, hop - 1, q).wait_recv()
                if hop < 3 or q == way:
                    go(ring_out(way, hop, q))
                go(to_twin(hop if way == 0 else NY - hop, q, core))

    def from_twin(*backs):
        for back in backs:
            for q in range(2):
                to_twin(back, q, 1 - core).wait_recv()

    for q in range(2):
        for way in range(2):
            go(ring_out(way, 0, q))
    for q in range(2):
        go(to_twin(0, q, core))
    pass_on(1)
    pass_on(2)
    from_twin(0, 1, 7, 2, 6)

    step = 256

    def chip_block(at, start, count, k):
        first = pl.multiple_of((at % NY) * chip_rows + start, 8)
        return s_all[pl.ds(first, count), k]

    far = (y + 2) % 4
    strip = chip_rows // 4

    def gram_step(i, acc):
        k = pl.ds(pl.multiple_of(i * step, 128), step)
        cols = chip_block(y + NY - core, 0, chip_rows, k)
        one = dot(chip_block(y + core, 0, chip_rows, k), cols, ((1,), (1,)))
        two = dot(chip_block(y + core + 1, 0, chip_rows, k), cols, ((1,), (1,)))
        edge = chip_block(far + 4, strip * (2 * (y // 4) + core), strip, k)
        three = dot(edge, chip_block(far, 0, chip_rows, k), ((1,), (1,)))
        return acc[0] + one, acc[1] + two, acc[2] + three

    nothing = jnp.zeros((chip_rows, chip_rows), jnp.float32)
    sums = lax.fori_loop(0, wide // step, gram_step, (nothing, nothing, nothing[:strip]))
    g_part[NX - 1, GT - 1] = jnp.zeros((8, 128), jnp.float32)
    t = 0
    for value in sums:
        for r in range(0, value.shape[0], 8):
            g_part[t // GT, t % GT, :, :chip_rows] = value[r : r + 8]
            t += 1

    def stages(sems, part, landing, spread, place):
        xs, xr, zs, zr, ys, yr, gs, gr, ts, tr = sems

        def x_copies():
            return [
                copy_to(part.at[(x + d) % NX], landing.at[d - 1], xs.at[d - 1], xr.at[d - 1], at_x(d))
                for d in range(1, NX)
            ]

        def x_total():
            spread[z] = (part[x] + landing[0] + landing[1] + landing[2]) * (1.0 / total)

        def z_copies(sign):
            def make():
                refs = [spread.at[(z + sign * d + NZ) % NZ if sign else z] for d in range(1, NZ)]
                return [copy_to(r, r, zs.at[d], zr.at[d], at_z(d + 1)) for d, r in enumerate(refs)]

            return make

        def z_total():
            value = spread[0]
            for i in range(1, NZ):
                value = value + spread[i]
            place[core, y, x] = value

        def y_copies(sign):
            def make():
                refs = [place.at[core, (y + sign * d + NY) % NY, x] for d in range(1, NY)]
                return [copy_to(r, r, ys.at[d], yr.at[d], at_y(d + 1)) for d, r in enumerate(refs)]

            return make

        def g_copies(sign):
            def make():
                refs = [place.at[core, :, (x + sign * d + NX) % NX] for d in range(1, NX)]
                return [copy_to(r, r, gs.at[d], gr.at[d], at_x(d + 1)) for d, r in enumerate(refs)]

            return make

        def t_copies(which):
            def make():
                return [copy_to(place.at[which], place.at[which], ts.at[0], tr.at[0], twin)]

            return make

        return (
            Exchange(x_copies, x_copies), x_total,
            Exchange(z_copies(0), z_copies(-1)), z_total,
            Exchange(y_copies(0), y_copies(-1)),
            Exchange(g_copies(0), g_copies(-1)),
            Exchange(t_copies(core), t_copies(1 - core)),
        )

    gx, gx_total, gz, gz_total, gy, gg, gt = stages(sems[:10], g_part, g_x, g_z, g_all)
    cx, cx_total, cz, cz_total, cy, cg, ct = stages(sems[10:], c_part, c_x, c_z, c_all)

    gx.start()
    gx.arrive()
    gx_total()
    gz.start()
    pass_on(3)
    for way in range(2):
        ring_in(way, 3, way).wait_recv()
        go(to_twin(4, way, core))
    gz.arrive()
    gz_total()
    gy.start()
    own_a.wait()
    from_twin(5, 3, 4)

    def cross_step(i, acc):
        k = pl.ds(pl.multiple_of(i * step, 128), step)
        return acc + dot3(a_own[:, k], s_all[:, k], ((1,), (1,)))

    crosst = lax.fori_loop(0, wide // step, cross_step, jnp.zeros((rows, s_all.shape[0]), jnp.float32))
    for t in range(NX * CT):
        r, h = 8 * (t // 6), 128 * (t % 6)
        c_part[t // CT, t % CT] = crosst[r : r + 8, h : h + 128]
    cx.start()
    gy.arrive()
    gg.start()
    cx.arrive()
    cx_total()
    cz.start()
    gg.arrive()
    gt.start()
    gt.arrive()

    for chip in range(NY):
        for which in range(2):
            tiles = [g_all[which, chip, t // GT, t % GT][:, :chip_rows] for t in range(NX * GT - 1)]
            blocks = chip_rows // 8
            for b in range(2):
                at, col = (chip + which + b) % NY, (chip - which) % NY
                block = tiles[b * blocks : (b + 1) * blocks]
                if at < col:
                    flipped = jnp.concatenate(block, axis=0).T
                    block = [flipped[8 * r : 8 * r + 8] for r in range(blocks)]
                    at, col = col, at
                for r, tile in enumerate(block):
                    first = at * chip_rows + 8 * r
                    z_ref[first : first + 8, col * chip_rows : (col + 1) * chip_rows] = tile
            col = (chip + 2) % 4
            for r, tile in enumerate(tiles[2 * blocks :]):
                first = (col + 4) * chip_rows + strip * (2 * (chip // 4) + which) + 8 * r
                z_ref[first : first + 8, col * chip_rows : (col + 1) * chip_rows] = tile

    def between(k):
        @pl.when(k == 1)
        def _():
            cz.arrive()
            cz_total()
            cy.start()

        @pl.when(k == 3)
        def _():
            cy.arrive()
            cg.start()

        @pl.when(k == 5)
        def _():
            cg.arrive()
            ct.start()

    invert_lower(z_ref, d_ref, m_ref, between)

    lower = z_ref[pl.ds(pl.multiple_of(mode * rows, 8), rows), :]

    @pl.loop(0, wide // step)
    def _(i):
        k = pl.ds(pl.multiple_of(i * step, 128), step)
        ortho_ref[:, k] = dot3(lower, s_all[:, k], ((1,), (0,)))

    ct.arrive()
    for m in range(2 * NY):
        for t in range(NX * CT):
            r, h = m * rows + 8 * (t // 6), 128 * (t % 6)
            ct_ref[r : r + 8, h : h + 128] = c_all[m % 2, m // 2, t // CT, t % CT]
    half = dot3(lower, ct_ref[...], ((1,), (1,)))
    proj_ref[...] = dot3(half, z_ref[...], ((1,), (1,)))
    for c in pending:
        c.wait_send()
    for e in (gx, gz, gy, gg, gt, cx, cz, cy, cg, ct):
        e.sent()


def per_device(subspace, applied):
    rows, wide = subspace.shape
    n = rows * lax.axis_size("modes")
    f32 = jnp.float32
    dma = pltpu.SemaphoreType.DMA
    exchange = [dma((count,)) for count in (NX - 1, NZ - 1, NY - 1, NX - 1, 1) for _ in range(2)]

    def buffers(count):
        return [
            pltpu.VMEM((NX, count, 8, 128), f32),
            pltpu.VMEM((NX - 1, count, 8, 128), f32),
            pltpu.VMEM((NZ, count, 8, 128), f32),
            pltpu.VMEM((2, NY, NX, count, 8, 128), f32),
        ]

    return pl.pallas_call(
        kernel,
        out_shape=(
            jax.ShapeDtypeStruct((rows, wide), f32),
            jax.ShapeDtypeStruct((rows, n), f32),
        ),
        in_specs=[pl.BlockSpec(memory_space=pl.ANY)] * 2,
        out_specs=[pl.BlockSpec(memory_space=pltpu.VMEM)] * 2,
        scratch_shapes=[
            pltpu.VMEM((n, wide), f32),
            pltpu.VMEM((rows, wide), f32),
            *buffers(GT),
            *buffers(CT),
            pltpu.VMEM((n, n), f32),
            pltpu.VMEM((n, n), f32),
            pltpu.VMEM((B, B), f32),
            pltpu.VMEM((B, B), f32),
            dma((2,)),
            *[dma((2, 4, 2)) for _ in range(2)],
            *[dma((NY, 2)) for _ in range(2)],
            *exchange,
            *exchange,
        ],
        compiler_params=pltpu.CompilerParams(
            collective_id=0, has_side_effects=True, vmem_limit_bytes=56 * 2**20
        ),
        name="cholesky_qr",
    )(subspace, applied)


def solution(mesh):
    return jax.shard_map(
        per_device,
        mesh=mesh,
        in_specs=(P("modes", "atoms"), P("modes", "atoms")),
        out_specs=(P("modes", "atoms"), P("modes", None)),
        check_vma=False,
    )
```

```python
import jax
import jax.numpy as jnp
from jax import lax
from jax.experimental import pallas as pl
from jax.experimental.pallas import tpu as pltpu
from jax.sharding import PartitionSpec as P

MESH = pl.DeviceIdType.MESH
NX, NY, NZ = 4, 8, 8
GT, CT = 7, 9

B = 128
PANEL, STRIP = 32, 16
HI = lax.Precision.HIGHEST


def lane_bcast(v, j):
    return jnp.broadcast_to(v[:, j : j + 1], v.shape)


def row_bcast(v, j):
    return jnp.broadcast_to(v[j : j + 1, :], v.shape)


def factor_block(d_ref, m_ref):
    lane = lax.broadcasted_iota(jnp.int32, (8, B), 1)
    sub = lax.broadcasted_iota(jnp.int32, (8, B), 0)
    for s in range(B // 8):
        m_ref[8 * s : 8 * s + 8, :] = jnp.where(lane == sub + 8 * s, 1.0, 0.0)
    n = PANEL // 8
    for p0 in range(0, B, PANEL):
        d = [d_ref[p0 + 8 * g : p0 + 8 * g + 8, :] for g in range(n)]
        m = [m_ref[p0 + 8 * g : p0 + 8 * g + 8, :] for g in range(n)]
        for s0 in range(0, n, STRIP // 8):
            r0 = p0 + 8 * s0
            col = {g: [lane_bcast(d[g], r0 + k) for k in range(STRIP)] for g in range(s0, n)}
            scale = {}
            for j in range(STRIP):
                s, jj = s0 + j // 8, j % 8
                pivot = row_bcast(col[s][j], jj)
                inv = 1.0 / pivot
                root = lax.rsqrt(pivot)
                scale[s] = root if jj == 0 else jnp.where(sub >= jj, root, scale[s])
                dj = row_bcast(d[s], jj) * inv
                mj = row_bcast(m[s], jj) * inv
                for k in range(j + 1, STRIP):
                    f = row_bcast(col[s][k], jj) * inv
                    for g in range(s, n):
                        if g > s or jj < 7:
                            col[g][k] = col[g][k] - col[g][j] * f
                for g in range(s, n):
                    c = col[g][j]
                    if g == s:
                        if jj == 7:
                            continue
                        c = jnp.where(sub > jj, c, 0.0)
                    d[g] = d[g] - c * dj
                    m[g] = m[g] - c * mj
            for s in range(s0, s0 + STRIP // 8):
                d[s] = d[s] * scale[s]
                m[s] = m[s] * scale[s]
        for g in range(n):
            m_ref[p0 + 8 * g : p0 + 8 * g + 8, :] = m[g]
        if p0 + PANEL < B:
            r = jnp.concatenate(d, axis=0)
            q = jnp.concatenate(m, axis=0)
            t = r.T[p0 + PANEL :, :]
            d_ref[p0 + PANEL :, :] -= dot(t, r, ((1,), (0,)))
            m_ref[p0 + PANEL :, :] -= dot(t, q, ((1,), (0,)))


def dot(a, b, dims):
    return lax.dot_general(a, b, (dims, ((), ())), precision=HI, preferred_element_type=jnp.float32)


def dot3(a, b, dims):
    bf, f32 = jnp.bfloat16, jnp.float32
    ah, bh = a.astype(bf), b.astype(bf)
    al, bl = (a - ah.astype(f32)).astype(bf), (b - bh.astype(f32)).astype(bf)

    def one(p, q):
        return lax.dot_general(p, q, (dims, ((), ())), preferred_element_type=f32)

    return one(ah, bh) + (one(al, bh) + one(ah, bl))


def invert_lower(z_ref, d_ref, m_ref, between):
    n = z_ref.shape[0]
    row = lax.broadcasted_iota(jnp.int32, (B, B), 0)
    lane = lax.broadcasted_iota(jnp.int32, (B, B), 1)

    def inverse_of_block(k):
        d = z_ref[k * B : (k + 1) * B, k * B : (k + 1) * B]
        d_ref[k] = jnp.where(row >= lane, d, d.T)
        factor_block(d_ref.at[k], m_ref.at[k])
        return m_ref[k]

    following = inverse_of_block(0)
    for k in range(n // B):
        between(k)
        lo, hi = k * B, (k + 1) * B
        m = following
        if hi < n:
            r = dot(m, z_ref[hi:, lo:hi], ((1,), (1,)))
            rt = r.T
            z_ref[hi : hi + B, hi : hi + B] -= dot(rt[:B], r[:, :B], ((1,), (0,)))
            following = inverse_of_block(k + 1)
            if hi + B < n:
                z_ref[hi + B :, hi : hi + B] -= dot(rt[B:], r[:, :B], ((1,), (0,)))
            for c in range(hi + B, n, 2 * B):
                e = min(c + 2 * B, n)
                z_ref[c:, c:e] -= dot(rt[c - hi :], r[:, c - hi : e - hi], ((1,), (0,)))
            z_ref[lo:hi, hi:] = jnp.zeros((B, n - hi), jnp.float32)
        if k:
            w = dot(m, z_ref[lo:hi, :lo], ((1,), (0,)))
            z_ref[lo:hi, :lo] = w
            if hi < n:
                z_ref[hi:, :lo] -= dot(rt, w, ((1,), (0,)))
        z_ref[lo:hi, lo:hi] = m
        if hi < n:
            z_ref[hi:, lo:hi] = -dot(rt, m, ((1,), (0,)))


def copy_to(src, dst, send, recv, device):
    return pltpu.make_async_remote_copy(
        src_ref=src, dst_ref=dst, send_sem=send, recv_sem=recv, device_id=device, device_id_type=MESH
    )


class Spread:
    def __init__(self, place, sems, me, at_x, at_y, twin):
        self.place, self.sems, self.me = place, sems, me
        self.at_x, self.at_y, self.twin = at_x, at_y, twin

    def part(self, back_y, back_x, other=False):
        core, y, x = self.me
        which = 1 - core if other else core
        return self.place.at[which, (y + NY - back_y) % NY, (x + NX - back_x) % NX]

    def along_y(self, d, arriving=False):
        ys, yr = self.sems[:2]
        ref = self.part(d if arriving else 0, 0)
        return copy_to(ref, ref, ys.at[d - 1], yr.at[d - 1], self.at_y(d))

    def along_x(self, back_y, d, arriving=False):
        xs, xr = self.sems[2:4]
        ref = self.part(back_y, d if arriving else 0)
        return copy_to(ref, ref, xs.at[back_y, d - 1], xr.at[back_y, d - 1], self.at_x(d))

    def to_twin(self, back_y, back_x, arriving=False):
        ts, tr = self.sems[4:]
        ref = self.part(back_y, back_x, arriving)
        return copy_to(ref, ref, ts.at[back_y, back_x], tr.at[back_y, back_x], self.twin)

    def pass_on(self, back_y):
        for d in range(1, NX):
            self.along_x(back_y, d).start()
        self.to_twin(back_y, 0).start()

    def start(self):
        for d in range(1, NY):
            self.along_y(d).start()
        self.pass_on(0)

    def forward(self, *backs):
        for back in backs:
            self.along_y(back, arriving=True).wait_recv()
            self.pass_on(back)

    def collect(self, *backs):
        for back in backs:
            for d in range(1, NX):
                self.along_x(back, d, arriving=True).wait_recv()
                self.to_twin(back, d).start()

    def arrive(self):
        for back_y in range(NY):
            for back_x in range(NX):
                self.to_twin(back_y, back_x, arriving=True).wait_recv()

    def sent(self):
        for d in range(1, NY):
            self.along_y(d).wait_send()
        for back_y in range(NY):
            for d in range(1, NX):
                self.along_x(back_y, d).wait_send()
            for back_x in range(NX):
                self.to_twin(back_y, back_x).wait_send()


class Exchange:
    def __init__(self, out, arriving):
        self.out, self.arriving = out, arriving

    def start(self):
        for c in self.out():
            c.start()

    def arrive(self):
        for c in self.arriving():
            c.wait_recv()

    def sent(self):
        for c in self.out():
            c.wait_send()


def kernel(
    s_hbm, a_hbm, ortho_ref, proj_ref,
    s_all, a_own, g_part, g_x, g_z, g_all, c_part, c_x, c_z, c_all, z_ref, ct_ref, d_ref, m_ref,
    load_sem, ring_send, ring_recv, twin_send, twin_recv, *sems,
):
    atom, mode = lax.axis_index("atoms"), lax.axis_index("modes")
    z, x = atom // NX, atom % NX
    y, core = mode // 2, mode % 2
    rows, wide = s_hbm.shape
    half_rows = rows // 2
    chip_rows = 2 * rows
    total = wide * NX * NZ

    def at_x(d):
        return (z * NX + (x + d) % NX, mode)

    def at_y(d):
        return (atom, ((y + d) % NY) * 2 + core)

    def at_z(d):
        return (((z + d) % NZ) * NX + x, mode)

    twin = (atom, y * 2 + (1 - core))

    barrier = pltpu.get_barrier_semaphore()
    peers = [at_z(d) for d in range(1, NZ)] + [at_y(d) for d in range(1, NY)]
    peers += [at_x(d) for d in range(1, NX)] + [twin]
    for peer in peers:
        pl.semaphore_signal(barrier, inc=1, device_id=peer, device_id_type=MESH)
    own_s = pltpu.make_async_copy(
        s_hbm, s_all.at[pl.ds(pl.multiple_of(mode * rows, 8), rows), :], load_sem.at[0]
    )
    own_a = pltpu.make_async_copy(a_hbm, a_own, load_sem.at[1])
    own_s.start()
    own_a.start()
    own_s.wait()
    pl.semaphore_wait(barrier, len(peers))

    pending = []

    def go(copy):
        copy.start()
        pending.append(copy)

    def piece(back, which, q):
        start = (((y + NY - back) % NY) * 2 + which) * rows + q * half_rows
        return s_all.at[pl.ds(pl.multiple_of(start, 8), half_rows), :]

    def ring(way, hop, q, back):
        ref = piece(back, core, q)
        sems = ring_send.at[way, hop, q], ring_recv.at[way, hop, q]
        return copy_to(ref, ref, *sems, at_y(1 if way == 0 else NY - 1))

    def ring_out(way, hop, q):
        return ring(way, hop, q, hop if way == 0 else (NY - hop) % NY)

    def ring_in(way, hop, q):
        return ring(way, hop, q, hop + 1 if way == 0 else NY - hop - 1)

    def to_twin(back, q, which):
        ref = piece(back, which, q)
        return copy_to(ref, ref, twin_send.at[back, q], twin_recv.at[back, q], twin)

    def pass_on(hop):
        for q in range(2):
            for way in range(2):
                ring_in(way, hop - 1, q).wait_recv()
                if hop < 3 or q == way:
                    go(ring_out(way, hop, q))
                go(to_twin(hop if way == 0 else NY - hop, q, core))

    def from_twin(*backs):
        for back in backs:
            for q in range(2):
                to_twin(back, q, 1 - core).wait_recv()

    for q in range(2):
        for way in range(2):
            go(ring_out(way, 0, q))
    for q in range(2):
        go(to_twin(0, q, core))
    pass_on(1)
    pass_on(2)
    from_twin(0, 1, 7, 2, 6)

    step = 256

    def chip_block(at, start, count, k):
        first = pl.multiple_of((at % NY) * chip_rows + start, 8)
        return s_all[pl.ds(first, count), k]

    far = (y + 2) % 4
    strip = chip_rows // 4

    def gram_step(i, acc):
        k = pl.ds(pl.multiple_of(i * step, 128), step)
        cols = chip_block(y + NY - core, 0, chip_rows, k)
        both = [chip_block(y + core + b, 0, chip_rows, k) for b in range(2)]
        main = dot(jnp.concatenate(both, axis=0), cols, ((1,), (1,)))
        edge = chip_block(far + 4, strip * (2 * (y // 4) + core), strip, k)
        side = dot(edge, chip_block(far, 0, chip_rows, k), ((1,), (1,)))
        return acc[0] + main, acc[1] + side

    nothing = jnp.zeros((2 * chip_rows, chip_rows), jnp.float32)
    sums = lax.fori_loop(0, wide // step, gram_step, (nothing, nothing[:strip]), unroll=2)
    g_part[NX - 1, GT - 1] = jnp.zeros((8, 128), jnp.float32)
    t = 0
    for value in sums:
        for r in range(0, value.shape[0], 8):
            g_part[t // GT, t % GT, :, :chip_rows] = value[r : r + 8]
            t += 1

    def stages(sems, part, landing, spread, place):
        xs, xr, zs, zr, *rest = sems

        def x_copies():
            return [
                copy_to(part.at[(x + d) % NX], landing.at[d - 1], xs.at[d - 1], xr.at[d - 1], at_x(d))
                for d in range(1, NX)
            ]

        def x_total():
            spread[z] = (part[x] + landing[0] + landing[1] + landing[2]) * (1.0 / total)

        def z_copies(sign):
            def make():
                refs = [spread.at[(z + sign * d + NZ) % NZ if sign else z] for d in range(1, NZ)]
                return [copy_to(r, r, zs.at[d], zr.at[d], at_z(d + 1)) for d, r in enumerate(refs)]

            return make

        def z_total():
            value = spread[0]
            for i in range(1, NZ):
                value = value + spread[i]
            place[core, y, x] = value

        return (
            Exchange(x_copies, x_copies), x_total,
            Exchange(z_copies(0), z_copies(-1)), z_total,
            Spread(place, rest, (core, y, x), at_x, at_y, twin),
        )

    gx, gx_total, gz, gz_total, g_spread = stages(sems[:10], g_part, g_x, g_z, g_all)
    cx, cx_total, cz, cz_total, c_spread = stages(sems[10:], c_part, c_x, c_z, c_all)

    gx.start()
    gx.arrive()
    gx_total()
    gz.start()
    pass_on(3)
    for way in range(2):
        ring_in(way, 3, way).wait_recv()
        go(to_twin(4, way, core))
    gz.arrive()
    gz_total()
    g_spread.start()
    own_a.wait()
    from_twin(5, 3, 4)

    def cross_step(i, acc):
        k = pl.ds(pl.multiple_of(i * step, 128), step)
        return acc + dot3(a_own[:, k], s_all[:, k], ((1,), (1,)))

    crosst = lax.fori_loop(0, wide // step, cross_step, jnp.zeros((rows, s_all.shape[0]), jnp.float32))
    for t in range(NX * CT):
        r, h = 8 * (t // 6), 128 * (t % 6)
        c_part[t // CT, t % CT] = crosst[r : r + 8, h : h + 128]
    cx.start()
    g_spread.forward(1, 7, 2, 6, 3, 5, 4)
    cx.arrive()
    cx_total()
    cz.start()
    g_spread.collect(0, 1, 7, 2, 6, 3, 5, 4)
    g_spread.arrive()

    for chip in range(NY):
        for which in range(2):
            tiles = [g_all[which, chip, t // GT, t % GT][:, :chip_rows] for t in range(NX * GT - 1)]
            blocks = chip_rows // 8
            for b in range(2):
                at, col = (chip + which + b) % NY, (chip - which) % NY
                block = tiles[b * blocks : (b + 1) * blocks]
                if at < col:
                    flipped = jnp.concatenate(block, axis=0).T
                    block = [flipped[8 * r : 8 * r + 8] for r in range(blocks)]
                    at, col = col, at
                for r, tile in enumerate(block):
                    first = at * chip_rows + 8 * r
                    z_ref[first : first + 8, col * chip_rows : (col + 1) * chip_rows] = tile
            col = (chip + 2) % 4
            for r, tile in enumerate(tiles[2 * blocks :]):
                first = (col + 4) * chip_rows + strip * (2 * (chip // 4) + which) + 8 * r
                z_ref[first : first + 8, col * chip_rows : (col + 1) * chip_rows] = tile

    def between(k):
        if k == 0:
            cz.arrive()
            cz_total()
            c_spread.start()
        if k == 1:
            c_spread.forward(1, 7, 2, 6)
        if k == 2:
            c_spread.forward(3, 5, 4)
        if k == 4:
            c_spread.collect(0, 1, 7)

    invert_lower(z_ref, d_ref, m_ref, between)

    lower = z_ref[pl.ds(pl.multiple_of(mode * rows, 8), rows), :]

    for i in range(0, wide, step):
        ortho_ref[:, i : i + step] = dot3(lower, s_all[:, i : i + step], ((1,), (0,)))
        if i == 0:
            c_spread.collect(2, 6, 3, 5, 4)

    c_spread.arrive()
    for m in range(2 * NY):
        for t in range(NX * CT):
            r, h = m * rows + 8 * (t // 6), 128 * (t % 6)
            ct_ref[r : r + 8, h : h + 128] = c_all[m % 2, m // 2, t // CT, t % CT]
    half = dot3(lower, ct_ref[...], ((1,), (1,)))
    proj_ref[...] = dot3(half, z_ref[...], ((1,), (1,)))
    for c in pending:
        c.wait_send()
    for e in (gx, gz, g_spread, cx, cz, c_spread):
        e.sent()


def per_device(subspace, applied):
    rows, wide = subspace.shape
    n = rows * lax.axis_size("modes")
    f32 = jnp.float32
    dma = pltpu.SemaphoreType.DMA
    shapes = ((NX - 1,), (NZ - 1,), (NY - 1,), (NY, NX - 1), (NY, NX))
    exchange = [dma(shape) for shape in shapes for _ in range(2)]

    def buffers(count):
        return [
            pltpu.VMEM((NX, count, 8, 128), f32),
            pltpu.VMEM((NX - 1, count, 8, 128), f32),
            pltpu.VMEM((NZ, count, 8, 128), f32),
            pltpu.VMEM((2, NY, NX, count, 8, 128), f32),
        ]

    return pl.pallas_call(
        kernel,
        out_shape=(
            jax.ShapeDtypeStruct((rows, wide), f32),
            jax.ShapeDtypeStruct((rows, n), f32),
        ),
        in_specs=[pl.BlockSpec(memory_space=pl.ANY)] * 2,
        out_specs=[pl.BlockSpec(memory_space=pltpu.VMEM)] * 2,
        scratch_shapes=[
            pltpu.VMEM((n, wide), f32),
            pltpu.VMEM((rows, wide), f32),
            *buffers(GT),
            *buffers(CT),
            pltpu.VMEM((n, n), f32),
            pltpu.VMEM((n, n), f32),
            pltpu.VMEM((n // B, B, B), f32),
            pltpu.VMEM((n // B, B, B), f32),
            dma((2,)),
            *[dma((2, 4, 2)) for _ in range(2)],
            *[dma((NY, 2)) for _ in range(2)],
            *exchange,
            *exchange,
        ],
        compiler_params=pltpu.CompilerParams(
            collective_id=0, has_side_effects=True, vmem_limit_bytes=56 * 2**20
        ),
        name="cholesky_qr",
    )(subspace, applied)


def solution(mesh):
    return jax.shard_map(
        per_device,
        mesh=mesh,
        in_specs=(P("modes", "atoms"), P("modes", "atoms")),
        out_specs=(P("modes", "atoms"), P("modes", None)),
        check_vma=False,
    )
```

```python
import jax
import jax.numpy as jnp
from jax import lax
from jax.experimental import pallas as pl
from jax.experimental.pallas import tpu as pltpu
from jax.sharding import PartitionSpec as P

MESH = pl.DeviceIdType.MESH
NX, NY, NZ = 4, 8, 8
GT, CT = 7, 9

B = 128
PANEL, STRIP = 32, 16
HI = lax.Precision.HIGHEST


def lane_bcast(v, j):
    return jnp.broadcast_to(v[:, j : j + 1], v.shape)


def row_bcast(v, j):
    return jnp.broadcast_to(v[j : j + 1, :], v.shape)


def factor_block(d_ref, m_ref):
    lane = lax.broadcasted_iota(jnp.int32, (8, B), 1)
    sub = lax.broadcasted_iota(jnp.int32, (8, B), 0)
    for s in range(B // 8):
        m_ref[8 * s : 8 * s + 8, :] = jnp.where(lane == sub + 8 * s, 1.0, 0.0)
    n = PANEL // 8
    for p0 in range(0, B, PANEL):
        d = [d_ref[p0 + 8 * g : p0 + 8 * g + 8, :] for g in range(n)]
        m = [m_ref[p0 + 8 * g : p0 + 8 * g + 8, :] for g in range(n)]
        for s0 in range(0, n, STRIP // 8):
            r0 = p0 + 8 * s0
            col = {g: [lane_bcast(d[g], r0 + k) for k in range(STRIP)] for g in range(s0, n)}
            scale = {}
            for j in range(STRIP):
                s, jj = s0 + j // 8, j % 8
                pivot = row_bcast(col[s][j], jj)
                inv = 1.0 / pivot
                root = lax.rsqrt(pivot)
                scale[s] = root if jj == 0 else jnp.where(sub >= jj, root, scale[s])
                dj = row_bcast(d[s], jj) * inv
                mj = row_bcast(m[s], jj) * inv
                for k in range(j + 1, STRIP):
                    f = row_bcast(col[s][k], jj) * inv
                    for g in range(s, n):
                        if g > s or jj < 7:
                            col[g][k] = col[g][k] - col[g][j] * f
                for g in range(s, n):
                    c = col[g][j]
                    if g == s:
                        if jj == 7:
                            continue
                        c = jnp.where(sub > jj, c, 0.0)
                    d[g] = d[g] - c * dj
                    m[g] = m[g] - c * mj
            for s in range(s0, s0 + STRIP // 8):
                d[s] = d[s] * scale[s]
                m[s] = m[s] * scale[s]
        for g in range(n):
            m_ref[p0 + 8 * g : p0 + 8 * g + 8, :] = m[g]
        if p0 + PANEL < B:
            r = jnp.concatenate(d, axis=0)
            q = jnp.concatenate(m, axis=0)
            t = r.T[p0 + PANEL :, :]
            d_ref[p0 + PANEL :, :] -= dot(t, r, ((1,), (0,)))
            m_ref[p0 + PANEL :, :] -= dot(t, q, ((1,), (0,)))


def dot(a, b, dims):
    return lax.dot_general(a, b, (dims, ((), ())), precision=HI, preferred_element_type=jnp.float32)


def dot3(a, b, dims):
    bf, f32 = jnp.bfloat16, jnp.float32
    ah, bh = a.astype(bf), b.astype(bf)
    al, bl = (a - ah.astype(f32)).astype(bf), (b - bh.astype(f32)).astype(bf)

    def one(p, q):
        return lax.dot_general(p, q, (dims, ((), ())), preferred_element_type=f32)

    return one(ah, bh) + (one(al, bh) + one(ah, bl))


def invert_lower(z_ref, d_ref, m_ref, between):
    n = z_ref.shape[0]
    row = lax.broadcasted_iota(jnp.int32, (B, B), 0)
    lane = lax.broadcasted_iota(jnp.int32, (B, B), 1)

    def inverse_of_block(k):
        d = z_ref[k * B : (k + 1) * B, k * B : (k + 1) * B]
        d_ref[k] = jnp.where(row >= lane, d, d.T)
        factor_block(d_ref.at[k], m_ref.at[k])
        return m_ref[k]

    following = inverse_of_block(0)
    for k in range(n // B):
        between(k)
        lo, hi = k * B, (k + 1) * B
        m = following
        if hi < n:
            r = dot(m, z_ref[hi:, lo:hi], ((1,), (1,)))
            rt = r.T
            z_ref[hi : hi + B, hi : hi + B] -= dot(rt[:B], r[:, :B], ((1,), (0,)))
            following = inverse_of_block(k + 1)
            if hi + B < n:
                z_ref[hi + B :, hi : hi + B] -= dot(rt[B:], r[:, :B], ((1,), (0,)))
            for c in range(hi + B, n, 2 * B):
                e = min(c + 2 * B, n)
                z_ref[c:, c:e] -= dot(rt[c - hi :], r[:, c - hi : e - hi], ((1,), (0,)))
            z_ref[lo:hi, hi:] = jnp.zeros((B, n - hi), jnp.float32)
        if k:
            w = dot(m, z_ref[lo:hi, :lo], ((1,), (0,)))
            z_ref[lo:hi, :lo] = w
            if hi < n:
                z_ref[hi:, :lo] -= dot(rt, w, ((1,), (0,)))
        z_ref[lo:hi, lo:hi] = m
        if hi < n:
            z_ref[hi:, lo:hi] = -dot(rt, m, ((1,), (0,)))


def copy_to(src, dst, send, recv, device):
    return pltpu.make_async_remote_copy(
        src_ref=src, dst_ref=dst, send_sem=send, recv_sem=recv, device_id=device, device_id_type=MESH
    )


def slot_of(back):
    over = back // (NY // 2 + 1)
    return (1 - over) * (2 * back - (back + NY - 1) // NY) + over * 2 * (NY - back)


class Spread:
    GROUPS = (5, 3)

    def __init__(self, place, sems, me, at_x, at_y, twin):
        self.place, self.sems, self.me = place, sems, me
        self.at_x, self.at_y, self.twin = at_x, at_y, twin

    def along_y(self, d, arriving=False):
        ys, yr = self.sems[:2]
        core, _, x = self.me
        return copy_to(
            self.place.at[core, 0, x], self.place.at[core, slot_of(d), x], ys.at[d - 1], yr.at[d - 1], self.at_y(d)
        )

    def group(self, g, back_x, other=False):
        core, _, x = self.me
        which = 1 - core if other else core
        slots = pl.ds(sum(self.GROUPS[:g]), self.GROUPS[g])
        return self.place.at[which, slots, (x + NX - back_x) % NX]

    def along_x(self, g, d, arriving=False):
        xs, xr = self.sems[2:4]
        ref = self.group(g, d if arriving else 0)
        return copy_to(ref, ref, xs.at[g, d - 1], xr.at[g, d - 1], self.at_x(d))

    def to_twin(self, g, back_x, arriving=False):
        ts, tr = self.sems[4:]
        ref = self.group(g, back_x, arriving)
        return copy_to(ref, ref, ts.at[g, back_x], tr.at[g, back_x], self.twin)

    def start(self):
        for d in (1, 7, 2, 6, 3, 5, 4):
            self.along_y(d).start()

    def forward(self, g):
        for d in ((1, 7, 2, 6), (3, 5, 4))[g]:
            self.along_y(d, arriving=True).wait_recv()
        for d in (2, 1, 3):
            self.along_x(g, d).start()
        self.to_twin(g, 0).start()

    def collect(self, g):
        for d in (1, 3, 2):
            self.along_x(g, d, arriving=True).wait_recv()
            self.to_twin(g, d).start()

    def arrive(self):
        for g in range(2):
            for back_x in range(NX):
                self.to_twin(g, back_x, arriving=True).wait_recv()

    def sent(self):
        for d in range(1, NY):
            self.along_y(d).wait_send()
        for g in range(2):
            for d in range(1, NX):
                self.along_x(g, d).wait_send()
            for back_x in range(NX):
                self.to_twin(g, back_x).wait_send()


class Exchange:
    def __init__(self, out, arriving):
        self.out, self.arriving = out, arriving

    def start(self):
        for c in self.out():
            c.start()

    def arrive(self):
        for c in self.arriving():
            c.wait_recv()

    def sent(self):
        for c in self.out():
            c.wait_send()


def kernel(
    s_hbm, a_hbm, ortho_ref, proj_ref,
    s_all, a_own, g_part, g_x, g_z, g_all, c_part, c_x, c_z, c_all, z_ref, ct_ref, d_ref, m_ref,
    load_sem, ring_send, ring_recv, twin_send, twin_recv, *sems,
):
    atom, mode = lax.axis_index("atoms"), lax.axis_index("modes")
    z, x = atom // NX, atom % NX
    y, core = mode // 2, mode % 2
    rows, wide = s_hbm.shape
    half_rows = rows // 2
    chip_rows = 2 * rows
    total = wide * NX * NZ

    def at_x(d):
        return (z * NX + (x + d) % NX, mode)

    def at_y(d):
        return (atom, ((y + d) % NY) * 2 + core)

    def at_z(d):
        return (((z + d) % NZ) * NX + x, mode)

    twin = (atom, y * 2 + (1 - core))

    barrier = pltpu.get_barrier_semaphore()
    peers = [at_z(d) for d in range(1, NZ)] + [at_y(d) for d in range(1, NY)]
    peers += [at_x(d) for d in range(1, NX)] + [twin]
    for peer in peers:
        pl.semaphore_signal(barrier, inc=1, device_id=peer, device_id_type=MESH)
    own_s = pltpu.make_async_copy(
        s_hbm, s_all.at[pl.ds(pl.multiple_of(mode * rows, 8), rows), :], load_sem.at[0]
    )
    own_a = pltpu.make_async_copy(a_hbm, a_own, load_sem.at[1])
    own_s.start()
    own_a.start()
    own_s.wait()
    pl.semaphore_wait(barrier, len(peers))

    pending = []

    def go(copy):
        copy.start()
        pending.append(copy)

    def piece(back, which, q):
        start = (((y + NY - back) % NY) * 2 + which) * rows + q * half_rows
        return s_all.at[pl.ds(pl.multiple_of(start, 8), half_rows), :]

    def ring(way, hop, q, back):
        ref = piece(back, core, q)
        sems = ring_send.at[way, hop, q], ring_recv.at[way, hop, q]
        return copy_to(ref, ref, *sems, at_y(1 if way == 0 else NY - 1))

    def ring_out(way, hop, q):
        return ring(way, hop, q, hop if way == 0 else (NY - hop) % NY)

    def ring_in(way, hop, q):
        return ring(way, hop, q, hop + 1 if way == 0 else NY - hop - 1)

    def to_twin(back, q, which):
        ref = piece(back, which, q)
        return copy_to(ref, ref, twin_send.at[back, q], twin_recv.at[back, q], twin)

    def pass_on(hop):
        for q in range(2):
            for way in range(2):
                ring_in(way, hop - 1, q).wait_recv()
                if hop < 3 or q == way:
                    go(ring_out(way, hop, q))
                go(to_twin(hop if way == 0 else NY - hop, q, core))

    def from_twin(*backs):
        for back in backs:
            for q in range(2):
                to_twin(back, q, 1 - core).wait_recv()

    for q in range(2):
        for way in range(2):
            go(ring_out(way, 0, q))
    for q in range(2):
        go(to_twin(0, q, core))
    pass_on(1)
    pass_on(2)
    from_twin(0, 1, 7, 2, 6)

    step = 256

    def chip_block(at, start, count, k):
        first = pl.multiple_of((at % NY) * chip_rows + start, 8)
        return s_all[pl.ds(first, count), k]

    far = (y + 2) % 4
    strip = chip_rows // 4

    def gram_step(i, acc):
        k = pl.ds(pl.multiple_of(i * step, 128), step)
        cols = chip_block(y + NY - core, 0, chip_rows, k)
        both = [chip_block(y + core + b, 0, chip_rows, k) for b in range(2)]
        main = dot(jnp.concatenate(both, axis=0), cols, ((1,), (1,)))
        edge = chip_block(far + 4, strip * (2 * (y // 4) + core), strip, k)
        side = dot(edge, chip_block(far, 0, chip_rows, k), ((1,), (1,)))
        return acc[0] + main, acc[1] + side

    nothing = jnp.zeros((2 * chip_rows, chip_rows), jnp.float32)
    sums = lax.fori_loop(0, wide // step, gram_step, (nothing, nothing[:strip]), unroll=2)
    g_part[NX - 1, GT - 1] = jnp.zeros((8, 128), jnp.float32)
    t = 0
    for value in sums:
        for r in range(0, value.shape[0], 8):
            g_part[t // GT, t % GT, :, :chip_rows] = value[r : r + 8]
            t += 1

    def stages(sems, part, landing, spread, place):
        xs, xr, zs, zr, *rest = sems

        def x_copies():
            return [
                copy_to(part.at[(x + d) % NX], landing.at[d - 1], xs.at[d - 1], xr.at[d - 1], at_x(d))
                for d in range(1, NX)
            ]

        def x_total():
            spread[z] = (part[x] + landing[0] + landing[1] + landing[2]) * (1.0 / total)

        def z_copies(sign):
            def make():
                refs = [spread.at[(z + sign * d + NZ) % NZ if sign else z] for d in range(1, NZ)]
                return [copy_to(r, r, zs.at[d], zr.at[d], at_z(d + 1)) for d, r in enumerate(refs)]

            return make

        def z_total():
            value = spread[0]
            for i in range(1, NZ):
                value = value + spread[i]
            place[core, 0, x] = value

        return (
            Exchange(x_copies, x_copies), x_total,
            Exchange(z_copies(0), z_copies(-1)), z_total,
            Spread(place, rest, (core, y, x), at_x, at_y, twin),
        )

    gx, gx_total, gz, gz_total, g_spread = stages(sems[:10], g_part, g_x, g_z, g_all)
    cx, cx_total, cz, cz_total, c_spread = stages(sems[10:], c_part, c_x, c_z, c_all)

    gx.start()
    gx.arrive()
    gx_total()
    gz.start()
    pass_on(3)
    for way in range(2):
        ring_in(way, 3, way).wait_recv()
        go(to_twin(4, way, core))
    gz.arrive()
    gz_total()
    g_spread.start()
    own_a.wait()
    from_twin(5, 3, 4)

    def cross_step(i, acc):
        k = pl.ds(pl.multiple_of(i * step, 128), step)
        return acc + dot3(a_own[:, k], s_all[:, k], ((1,), (1,)))

    crosst = lax.fori_loop(0, wide // step, cross_step, jnp.zeros((rows, s_all.shape[0]), jnp.float32))
    for t in range(NX * CT):
        r, h = 8 * (t // 6), 128 * (t % 6)
        c_part[t // CT, t % CT] = crosst[r : r + 8, h : h + 128]
    cx.start()
    g_spread.forward(0)
    cx.arrive()
    cx_total()
    cz.start()
    g_spread.forward(1)
    g_spread.collect(0)
    g_spread.collect(1)
    cz.arrive()
    cz_total()
    c_spread.start()
    g_spread.arrive()

    slots = [slot_of((y + NY - chip) % NY) for chip in range(NY)]
    for chip in range(NY):
        for which in range(2):
            tiles = [g_all[which, slots[chip], t // GT, t % GT][:, :chip_rows] for t in range(NX * GT - 1)]
            blocks = chip_rows // 8
            for b in range(2):
                at, col = (chip + which + b) % NY, (chip - which) % NY
                block = tiles[b * blocks : (b + 1) * blocks]
                if at < col:
                    flipped = jnp.concatenate(block, axis=0).T
                    block = [flipped[8 * r : 8 * r + 8] for r in range(blocks)]
                    at, col = col, at
                for r, tile in enumerate(block):
                    first = at * chip_rows + 8 * r
                    z_ref[first : first + 8, col * chip_rows : (col + 1) * chip_rows] = tile
            col = (chip + 2) % 4
            for r, tile in enumerate(tiles[2 * blocks :]):
                first = (col + 4) * chip_rows + strip * (2 * (chip // 4) + which) + 8 * r
                z_ref[first : first + 8, col * chip_rows : (col + 1) * chip_rows] = tile

    def between(k):
        if k < 2:
            c_spread.forward(k)
        elif k > 3:
            c_spread.collect(k - 4)

    invert_lower(z_ref, d_ref, m_ref, between)

    lower = z_ref[pl.ds(pl.multiple_of(mode * rows, 8), rows), :]

    for i in range(0, wide, step):
        ortho_ref[:, i : i + step] = dot3(lower, s_all[:, i : i + step], ((1,), (0,)))

    c_spread.arrive()
    for m in range(2 * NY):
        for t in range(NX * CT):
            r, h = m * rows + 8 * (t // 6), 128 * (t % 6)
            ct_ref[r : r + 8, h : h + 128] = c_all[m % 2, slots[m // 2], t // CT, t % CT]
    half = dot3(lower, ct_ref[...], ((1,), (1,)))
    proj_ref[...] = dot3(half, z_ref[...], ((1,), (1,)))
    for c in pending:
        c.wait_send()
    for e in (gx, gz, g_spread, cx, cz, c_spread):
        e.sent()


def per_device(subspace, applied):
    rows, wide = subspace.shape
    n = rows * lax.axis_size("modes")
    f32 = jnp.float32
    dma = pltpu.SemaphoreType.DMA
    shapes = ((NX - 1,), (NZ - 1,), (NY - 1,), (2, NX - 1), (2, NX))
    exchange = [dma(shape) for shape in shapes for _ in range(2)]

    def buffers(count):
        return [
            pltpu.VMEM((NX, count, 8, 128), f32),
            pltpu.VMEM((NX - 1, count, 8, 128), f32),
            pltpu.VMEM((NZ, count, 8, 128), f32),
            pltpu.VMEM((2, NY, NX, count, 8, 128), f32),
        ]

    return pl.pallas_call(
        kernel,
        out_shape=(
            jax.ShapeDtypeStruct((rows, wide), f32),
            jax.ShapeDtypeStruct((rows, n), f32),
        ),
        in_specs=[pl.BlockSpec(memory_space=pl.ANY)] * 2,
        out_specs=[pl.BlockSpec(memory_space=pltpu.VMEM)] * 2,
        scratch_shapes=[
            pltpu.VMEM((n, wide), f32),
            pltpu.VMEM((rows, wide), f32),
            *buffers(GT),
            *buffers(CT),
            pltpu.VMEM((n, n), f32),
            pltpu.VMEM((n, n), f32),
            pltpu.VMEM((n // B, B, B), f32),
            pltpu.VMEM((n // B, B, B), f32),
            dma((2,)),
            *[dma((2, 4, 2)) for _ in range(2)],
            *[dma((NY, 2)) for _ in range(2)],
            *exchange,
            *exchange,
        ],
        compiler_params=pltpu.CompilerParams(
            collective_id=0, has_side_effects=True, vmem_limit_bytes=56 * 2**20
        ),
        name="cholesky_qr",
    )(subspace, applied)


def solution(mesh):
    return jax.shard_map(
        per_device,
        mesh=mesh,
        in_specs=(P("modes", "atoms"), P("modes", "atoms")),
        out_specs=(P("modes", "atoms"), P("modes", None)),
        check_vma=False,
    )
```

```python
import jax
import jax.numpy as jnp
from jax import lax
from jax.experimental import pallas as pl
from jax.experimental.pallas import tpu as pltpu
from jax.sharding import PartitionSpec as P

MESH = pl.DeviceIdType.MESH
NX, NY, NZ = 4, 8, 8
GT, CT = 7, 9

B = 128
PANEL, STRIP = 32, 16
HI = lax.Precision.HIGHEST


def lane_bcast(v, j):
    return jnp.broadcast_to(v[:, j : j + 1], v.shape)


def row_bcast(v, j):
    return jnp.broadcast_to(v[j : j + 1, :], v.shape)


def factor_block(d_ref, m_ref):
    lane = lax.broadcasted_iota(jnp.int32, (8, B), 1)
    sub = lax.broadcasted_iota(jnp.int32, (8, B), 0)
    for s in range(B // 8):
        m_ref[8 * s : 8 * s + 8, :] = jnp.where(lane == sub + 8 * s, 1.0, 0.0)
    n = PANEL // 8
    for p0 in range(0, B, PANEL):
        d = [d_ref[p0 + 8 * g : p0 + 8 * g + 8, :] for g in range(n)]
        m = [m_ref[p0 + 8 * g : p0 + 8 * g + 8, :] for g in range(n)]
        for s0 in range(0, n, STRIP // 8):
            r0 = p0 + 8 * s0
            col = {g: [lane_bcast(d[g], r0 + k) for k in range(STRIP)] for g in range(s0, n)}
            scale = {}
            for j in range(STRIP):
                s, jj = s0 + j // 8, j % 8
                pivot = row_bcast(col[s][j], jj)
                inv = 1.0 / pivot
                root = lax.rsqrt(pivot)
                scale[s] = root if jj == 0 else jnp.where(sub >= jj, root, scale[s])
                dj = row_bcast(d[s], jj) * inv
                mj = row_bcast(m[s], jj) * inv
                for k in range(j + 1, STRIP):
                    f = row_bcast(col[s][k], jj) * inv
                    for g in range(s, n):
                        if g > s or jj < 7:
                            col[g][k] = col[g][k] - col[g][j] * f
                for g in range(s, n):
                    c = col[g][j]
                    if g == s:
                        if jj == 7:
                            continue
                        c = jnp.where(sub > jj, c, 0.0)
                    d[g] = d[g] - c * dj
                    m[g] = m[g] - c * mj
            for s in range(s0, s0 + STRIP // 8):
                d[s] = d[s] * scale[s]
                m[s] = m[s] * scale[s]
        for g in range(n):
            m_ref[p0 + 8 * g : p0 + 8 * g + 8, :] = m[g]
        if p0 + PANEL < B:
            r = jnp.concatenate(d, axis=0)
            q = jnp.concatenate(m, axis=0)
            t = r.T[p0 + PANEL :, :]
            d_ref[p0 + PANEL :, :] -= dot(t, r, ((1,), (0,)))
            m_ref[p0 + PANEL :, :] -= dot(t, q, ((1,), (0,)))


def dot(a, b, dims):
    return lax.dot_general(a, b, (dims, ((), ())), precision=HI, preferred_element_type=jnp.float32)


def dot3(a, b, dims):
    bf, f32 = jnp.bfloat16, jnp.float32
    ah, bh = a.astype(bf), b.astype(bf)
    al, bl = (a - ah.astype(f32)).astype(bf), (b - bh.astype(f32)).astype(bf)

    def one(p, q):
        return lax.dot_general(p, q, (dims, ((), ())), preferred_element_type=f32)

    return one(ah, bh) + (one(al, bh) + one(ah, bl))


def invert_lower(z_ref, d_ref, m_ref, between):
    n = z_ref.shape[0]
    row = lax.broadcasted_iota(jnp.int32, (B, B), 0)
    lane = lax.broadcasted_iota(jnp.int32, (B, B), 1)

    def inverse_of_block(k):
        d = z_ref[k * B : (k + 1) * B, k * B : (k + 1) * B]
        d_ref[k] = jnp.where(row >= lane, d, d.T)
        factor_block(d_ref.at[k], m_ref.at[k])
        return m_ref[k]

    following = inverse_of_block(0)
    for k in range(n // B):
        between(k)
        lo, hi = k * B, (k + 1) * B
        m = following
        if hi < n:
            r = dot(m, z_ref[hi:, lo:hi], ((1,), (1,)))
            rt = r.T
            z_ref[hi : hi + B, hi : hi + B] -= dot(rt[:B], r[:, :B], ((1,), (0,)))
            following = inverse_of_block(k + 1)
            if hi + B < n:
                z_ref[hi + B :, hi : hi + B] -= dot(rt[B:], r[:, :B], ((1,), (0,)))
            for c in range(hi + B, n, 2 * B):
                e = min(c + 2 * B, n)
                z_ref[c:, c:e] -= dot(rt[c - hi :], r[:, c - hi : e - hi], ((1,), (0,)))
            z_ref[lo:hi, hi:] = jnp.zeros((B, n - hi), jnp.float32)
        if k:
            w = dot(m, z_ref[lo:hi, :lo], ((1,), (0,)))
            z_ref[lo:hi, :lo] = w
            if hi < n:
                z_ref[hi:, :lo] -= dot(rt, w, ((1,), (0,)))
        z_ref[lo:hi, lo:hi] = m
        if hi < n:
            z_ref[hi:, lo:hi] = -dot(rt, m, ((1,), (0,)))


def copy_to(src, dst, send, recv, device):
    return pltpu.make_async_remote_copy(
        src_ref=src, dst_ref=dst, send_sem=send, recv_sem=recv, device_id=device, device_id_type=MESH
    )


def slot_of(back):
    over = back // (NY // 2 + 1)
    return (1 - over) * (2 * back - (back + NY - 1) // NY) + over * 2 * (NY - back)


class Spread:
    GROUPS = (5, 3)

    def __init__(self, place, sems, me, at_x, at_y, twin):
        self.place, self.sems, self.me = place, sems, me
        self.at_x, self.at_y, self.twin = at_x, at_y, twin

    def along_y(self, d, arriving=False):
        ys, yr = self.sems[:2]
        core, _, x = self.me
        return copy_to(
            self.place.at[core, 0, x], self.place.at[core, slot_of(d), x], ys.at[d - 1], yr.at[d - 1], self.at_y(d)
        )

    def group(self, g, back_x, other=False):
        core, _, x = self.me
        which = 1 - core if other else core
        slots = pl.ds(sum(self.GROUPS[:g]), self.GROUPS[g])
        return self.place.at[which, slots, (x + NX - back_x) % NX]

    def along_x(self, g, d, arriving=False):
        xs, xr = self.sems[2:4]
        ref = self.group(g, d if arriving else 0)
        return copy_to(ref, ref, xs.at[g, d - 1], xr.at[g, d - 1], self.at_x(d))

    def to_twin(self, g, back_x, arriving=False):
        ts, tr = self.sems[4:]
        ref = self.group(g, back_x, arriving)
        return copy_to(ref, ref, ts.at[g, back_x], tr.at[g, back_x], self.twin)

    def start(self):
        for d in (1, 7, 2, 6, 3, 5, 4):
            self.along_y(d).start()

    def forward(self, g):
        for d in ((1, 7, 2, 6), (3, 5, 4))[g]:
            self.along_y(d, arriving=True).wait_recv()
        for d in (2, 1, 3):
            self.along_x(g, d).start()
        self.to_twin(g, 0).start()

    def collect(self, g):
        for d in (1, 3, 2):
            self.along_x(g, d, arriving=True).wait_recv()
            self.to_twin(g, d).start()

    def arrive(self):
        for g in range(2):
            for back_x in range(NX):
                self.to_twin(g, back_x, arriving=True).wait_recv()

    def sent(self):
        for d in range(1, NY):
            self.along_y(d).wait_send()
        for g in range(2):
            for d in range(1, NX):
                self.along_x(g, d).wait_send()
            for back_x in range(NX):
                self.to_twin(g, back_x).wait_send()


class Exchange:
    def __init__(self, out, arriving):
        self.out, self.arriving = out, arriving

    def start(self):
        copies = self.out()
        far = (len(copies) + 1) / 2
        for i in sorted(range(len(copies)), key=lambda i: abs(i + 1 - far)):
            copies[i].start()

    def arrive(self):
        for c in self.arriving():
            c.wait_recv()

    def sent(self):
        for c in self.out():
            c.wait_send()


def kernel(
    s_hbm, a_hbm, ortho_ref, proj_ref,
    s_all, a_own, g_part, g_x, g_z, g_all, c_part, c_x, c_z, c_all, z_ref, ct_ref, d_ref, m_ref,
    load_sem, ring_send, ring_recv, twin_send, twin_recv, *sems,
):
    atom, mode = lax.axis_index("atoms"), lax.axis_index("modes")
    z, x = atom // NX, atom % NX
    y, core = mode // 2, mode % 2
    rows, wide = s_hbm.shape
    half_rows = rows // 2
    chip_rows = 2 * rows
    total = wide * NX * NZ

    def at_x(d):
        return (z * NX + (x + d) % NX, mode)

    def at_y(d):
        return (atom, ((y + d) % NY) * 2 + core)

    def at_z(d):
        return (((z + d) % NZ) * NX + x, mode)

    twin = (atom, y * 2 + (1 - core))

    barrier = pltpu.get_barrier_semaphore()
    peers = [at_z(d) for d in range(1, NZ)] + [at_y(d) for d in range(1, NY)]
    peers += [at_x(d) for d in range(1, NX)] + [twin]
    for peer in peers:
        pl.semaphore_signal(barrier, inc=1, device_id=peer, device_id_type=MESH)
    own_s = pltpu.make_async_copy(
        s_hbm, s_all.at[pl.ds(pl.multiple_of(mode * rows, 8), rows), :], load_sem.at[0]
    )
    own_a = pltpu.make_async_copy(a_hbm, a_own, load_sem.at[1])
    own_s.start()
    own_a.start()
    own_s.wait()
    pl.semaphore_wait(barrier, len(peers))

    pending = []

    def go(copy):
        copy.start()
        pending.append(copy)

    def piece(back, which, q):
        start = (((y + NY - back) % NY) * 2 + which) * rows + q * half_rows
        return s_all.at[pl.ds(pl.multiple_of(start, 8), half_rows), :]

    def ring(way, hop, q, back):
        ref = piece(back, core, q)
        sems = ring_send.at[way, hop, q], ring_recv.at[way, hop, q]
        return copy_to(ref, ref, *sems, at_y(1 if way == 0 else NY - 1))

    def ring_out(way, hop, q):
        return ring(way, hop, q, hop if way == 0 else (NY - hop) % NY)

    def ring_in(way, hop, q):
        return ring(way, hop, q, hop + 1 if way == 0 else NY - hop - 1)

    def to_twin(back, q, which):
        ref = piece(back, which, q)
        return copy_to(ref, ref, twin_send.at[back, q], twin_recv.at[back, q], twin)

    def pass_on(hop):
        for q in range(2):
            for way in range(2):
                ring_in(way, hop - 1, q).wait_recv()
                if hop < 3 or q == way:
                    go(ring_out(way, hop, q))
                go(to_twin(hop if way == 0 else NY - hop, q, core))

    def from_twin(*backs):
        for back in backs:
            for q in range(2):
                to_twin(back, q, 1 - core).wait_recv()

    for q in range(2):
        for way in range(2):
            go(ring_out(way, 0, q))
    for q in range(2):
        go(to_twin(0, q, core))
    pass_on(1)
    pass_on(2)
    from_twin(0, 1, 7, 2, 6)

    step = 256

    def chip_block(at, start, count, k):
        first = pl.multiple_of((at % NY) * chip_rows + start, 8)
        return s_all[pl.ds(first, count), k]

    far = (y + 2) % 4
    strip = chip_rows // 4

    def gram_step(i, acc):
        k = pl.ds(pl.multiple_of(i * step, 128), step)
        cols = chip_block(y + NY - core, 0, chip_rows, k)
        both = [chip_block(y + core + b, 0, chip_rows, k) for b in range(2)]
        main = dot(jnp.concatenate(both, axis=0), cols, ((1,), (1,)))
        edge = chip_block(far + 4, strip * (2 * (y // 4) + core), strip, k)
        side = dot(edge, chip_block(far, 0, chip_rows, k), ((1,), (1,)))
        return acc[0] + main, acc[1] + side

    nothing = jnp.zeros((2 * chip_rows, chip_rows), jnp.float32)
    sums = lax.fori_loop(0, wide // step, gram_step, (nothing, nothing[:strip]), unroll=2)
    g_part[NX - 1, GT - 1] = jnp.zeros((8, 128), jnp.float32)
    t = 0
    for value in sums:
        for r in range(0, value.shape[0], 8):
            g_part[t // GT, t % GT, :, :chip_rows] = value[r : r + 8]
            t += 1

    def stages(sems, part, landing, spread, place):
        xs, xr, zs, zr, *rest = sems

        def x_copies():
            return [
                copy_to(part.at[(x + d) % NX], landing.at[d - 1], xs.at[d - 1], xr.at[d - 1], at_x(d))
                for d in range(1, NX)
            ]

        def x_total():
            spread[z] = (part[x] + landing[0] + landing[1] + landing[2]) * (1.0 / total)

        def z_copies(sign):
            def make():
                refs = [spread.at[(z + sign * d + NZ) % NZ if sign else z] for d in range(1, NZ)]
                return [copy_to(r, r, zs.at[d], zr.at[d], at_z(d + 1)) for d, r in enumerate(refs)]

            return make

        def z_total():
            value = spread[0]
            for i in range(1, NZ):
                value = value + spread[i]
            place[core, 0, x] = value

        return (
            Exchange(x_copies, x_copies), x_total,
            Exchange(z_copies(0), z_copies(-1)), z_total,
            Spread(place, rest, (core, y, x), at_x, at_y, twin),
        )

    gx, gx_total, gz, gz_total, g_spread = stages(sems[:10], g_part, g_x, g_z, g_all)
    cx, cx_total, cz, cz_total, c_spread = stages(sems[10:], c_part, c_x, c_z, c_all)

    gx.start()
    gx.arrive()
    gx_total()
    gz.start()
    pass_on(3)
    for way in range(2):
        ring_in(way, 3, way).wait_recv()
        go(to_twin(4, way, core))
    gz.arrive()
    gz_total()
    g_spread.start()
    own_a.wait()
    from_twin(5, 3, 4)

    def cross_step(i, acc):
        k = pl.ds(pl.multiple_of(i * step, 128), step)
        return acc + dot3(a_own[:, k], s_all[:, k], ((1,), (1,)))

    crosst = lax.fori_loop(0, wide // step, cross_step, jnp.zeros((rows, s_all.shape[0]), jnp.float32))
    for t in range(NX * CT):
        r, h = 8 * (t // 6), 128 * (t % 6)
        c_part[t // CT, t % CT] = crosst[r : r + 8, h : h + 128]
    cx.start()
    g_spread.forward(0)
    cx.arrive()
    cx_total()
    cz.start()
    g_spread.forward(1)
    g_spread.collect(0)
    g_spread.collect(1)
    cz.arrive()
    cz_total()
    c_spread.start()
    g_spread.arrive()

    slots = [slot_of((y + NY - chip) % NY) for chip in range(NY)]
    for chip in range(NY):
        for which in range(2):
            tiles = [g_all[which, slots[chip], t // GT, t % GT][:, :chip_rows] for t in range(NX * GT - 1)]
            blocks = chip_rows // 8
            for b in range(2):
                at, col = (chip + which + b) % NY, (chip - which) % NY
                block = tiles[b * blocks : (b + 1) * blocks]
                if at < col:
                    flipped = jnp.concatenate(block, axis=0).T
                    block = [flipped[8 * r : 8 * r + 8] for r in range(blocks)]
                    at, col = col, at
                for r, tile in enumerate(block):
                    first = at * chip_rows + 8 * r
                    z_ref[first : first + 8, col * chip_rows : (col + 1) * chip_rows] = tile
            col = (chip + 2) % 4
            for r, tile in enumerate(tiles[2 * blocks :]):
                first = (col + 4) * chip_rows + strip * (2 * (chip // 4) + which) + 8 * r
                z_ref[first : first + 8, col * chip_rows : (col + 1) * chip_rows] = tile

    def between(k):
        if k < 2:
            c_spread.forward(k)
        elif k > 3:
            c_spread.collect(k - 4)

    invert_lower(z_ref, d_ref, m_ref, between)

    lower = z_ref[pl.ds(pl.multiple_of(mode * rows, 8), rows), :]

    for i in range(0, wide, step):
        ortho_ref[:, i : i + step] = dot3(lower, s_all[:, i : i + step], ((1,), (0,)))

    c_spread.arrive()
    for m in range(2 * NY):
        for t in range(NX * CT):
            r, h = m * rows + 8 * (t // 6), 128 * (t % 6)
            ct_ref[r : r + 8, h : h + 128] = c_all[m % 2, slots[m // 2], t // CT, t % CT]
    half = dot3(lower, ct_ref[...], ((1,), (1,)))
    proj_ref[...] = dot3(half, z_ref[...], ((1,), (1,)))
    for c in pending:
        c.wait_send()
    for e in (gx, gz, g_spread, cx, cz, c_spread):
        e.sent()


def per_device(subspace, applied):
    rows, wide = subspace.shape
    n = rows * lax.axis_size("modes")
    f32 = jnp.float32
    dma = pltpu.SemaphoreType.DMA
    shapes = ((NX - 1,), (NZ - 1,), (NY - 1,), (2, NX - 1), (2, NX))
    exchange = [dma(shape) for shape in shapes for _ in range(2)]

    def buffers(count):
        return [
            pltpu.VMEM((NX, count, 8, 128), f32),
            pltpu.VMEM((NX - 1, count, 8, 128), f32),
            pltpu.VMEM((NZ, count, 8, 128), f32),
            pltpu.VMEM((2, NY, NX, count, 8, 128), f32),
        ]

    return pl.pallas_call(
        kernel,
        out_shape=(
            jax.ShapeDtypeStruct((rows, wide), f32),
            jax.ShapeDtypeStruct((rows, n), f32),
        ),
        in_specs=[pl.BlockSpec(memory_space=pl.ANY)] * 2,
        out_specs=[pl.BlockSpec(memory_space=pltpu.VMEM)] * 2,
        scratch_shapes=[
            pltpu.VMEM((n, wide), f32),
            pltpu.VMEM((rows, wide), f32),
            *buffers(GT),
            *buffers(CT),
            pltpu.VMEM((n, n), f32),
            pltpu.VMEM((n, n), f32),
            pltpu.VMEM((n // B, B, B), f32),
            pltpu.VMEM((n // B, B, B), f32),
            dma((2,)),
            *[dma((2, 4, 2)) for _ in range(2)],
            *[dma((NY, 2)) for _ in range(2)],
            *exchange,
            *exchange,
        ],
        compiler_params=pltpu.CompilerParams(
            collective_id=0, has_side_effects=True, vmem_limit_bytes=56 * 2**20
        ),
        name="cholesky_qr",
    )(subspace, applied)


def solution(mesh):
    return jax.shard_map(
        per_device,
        mesh=mesh,
        in_specs=(P("modes", "atoms"), P("modes", "atoms")),
        out_specs=(P("modes", "atoms"), P("modes", None)),
        check_vma=False,
    )
```
